8 devices in a mesh: pp: 2 (over z, y), ep: 4 (over x, core).
Axes of the slice: x: 2, y: 2, z: 1, core: 2. Of those that a mesh axis runs over, the one named last changes fastest.
Arguments:
- x_fwd: bfloat16 [2, 8192, 512], P('pp', 'ep')
- x_bwd: bfloat16 [2, 8192, 512], P('pp', 'ep')
- dy_bwd: bfloat16 [2, 8192, 512], P('pp', 'ep')
- ids_fwd: int32 [2, 8192, 4], P('pp', 'ep')
- gate_fwd: bfloat16 [2, 8192, 4], P('pp', 'ep')
- ids_bwd: int32 [2, 8192, 4], P('pp', 'ep')
- gate_bwd: bfloat16 [2, 8192, 4], P('pp', 'ep')
- w_in: bfloat16 [2, 512, 1280], P('pp')
- w_out: bfloat16 [2, 1280, 512], P('pp')
- w_gate: bfloat16 [2, 16, 512, 1280], P('pp', 'ep')
- w_up: bfloat16 [2, 16, 512, 1280], P('pp', 'ep')
- w_down: bfloat16 [2, 16, 1280, 512], P('pp', 'ep')
Outputs:
- output 1: bfloat16 [2, 8192, 512], P('pp', 'ep')
- output 2: bfloat16 [2, 8192, 512], P('pp', 'ep')
- output 3: float32 [2, 16, 512, 1280], P('pp', 'ep')
- output 4: float32 [2, 16, 512, 1280], P('pp', 'ep')
- output 5: float32 [2, 16, 1280, 512], P('pp', 'ep')
All inputs are finite; a program needn't handle non-finite values.
Results may differ from the reference program's by a relative error of at most 0.0143664.
Values are sent between devices in bfloat16 or wider.
A program may use at most 1 GiB of HBM per device.

```python
import jax
import jax.numpy as jnp
from jax import lax

PP = 2
EP = 4
TOKENS = 2048
HIDDEN = 512
FF_DENSE = 1280
FF_EXPERT = 1280
EXPERTS = 16
TOP = 4
EPS_NORM = 1e-6
E_LOCAL = EXPERTS // EP
CAPACITY = 3 * TOKENS * TOP // EXPERTS
ROUTES = TOKENS * TOP


def draw_routes(rng_key):
    hot_dev = jax.random.randint(jax.random.fold_in(rng_key, 0), (), 0, EP)
    is_cold = (jnp.arange(EXPERTS) // E_LOCAL != hot_dev).astype(jnp.int32)
    weights = jnp.where(jnp.arange(EXPERTS) < E_LOCAL, 3 * (EP - 1), EP - 3).astype(jnp.int32)
    bounds = (ROUTES * jnp.cumsum(weights)) // (E_LOCAL * (EP - 1) * EP)
    counts = bounds - jnp.concatenate([jnp.zeros((1,), jnp.int32), bounds[:-1]])
    route_idx = jnp.arange(ROUTES)

    def one_source(src_dev):
        src_key = jax.random.fold_in(rng_key, src_dev + 1)
        key_order, key_tok = jax.random.split(src_key)
        score = is_cold * EXPERTS + jax.random.permutation(key_order, EXPERTS)
        exp_order = jnp.argsort(score).astype(jnp.int32)
        route_exp = jnp.repeat(exp_order, counts, total_repeat_length=ROUTES)
        tok_idx = jax.random.permutation(key_tok, TOKENS)[route_idx % TOKENS]
        return jnp.zeros((TOKENS, TOP), jnp.int32).at[tok_idx, route_idx // TOKENS].set(route_exp)

    return jax.vmap(one_source)(jnp.arange(EP)).reshape(EP * TOKENS, TOP)


def setup_inputs(seed: int = 0) -> dict:
    keys_all = jax.random.split(jax.random.key(seed), 12)
    act_shape = (PP, EP * TOKENS, HIDDEN)
    route_shape = (PP, EP * TOKENS, TOP)
    gate_scale = TOP ** -0.5
    x_fwd = jax.random.normal(keys_all[0], act_shape, jnp.float32).astype(jnp.bfloat16)
    x_bwd = jax.random.normal(keys_all[1], act_shape, jnp.float32).astype(jnp.bfloat16)
    dy_bwd = jax.random.normal(keys_all[2], act_shape, jnp.float32).astype(jnp.bfloat16)
    ids_fwd = jax.vmap(draw_routes)(jax.random.split(keys_all[3], PP))
    ids_bwd = jax.vmap(draw_routes)(jax.random.split(keys_all[4], PP))
    gate_fwd = (jax.random.uniform(keys_all[5], route_shape, jnp.float32, 0.5, 1.5) * gate_scale).astype(jnp.bfloat16)
    gate_bwd = (jax.random.uniform(keys_all[6], route_shape, jnp.float32, 0.5, 1.5) * gate_scale).astype(jnp.bfloat16)
    w_in = (jax.random.normal(keys_all[7], (PP, HIDDEN, FF_DENSE), jnp.float32) * HIDDEN ** -0.5).astype(jnp.bfloat16)
    w_out = (jax.random.normal(keys_all[8], (PP, FF_DENSE, HIDDEN), jnp.float32) * FF_DENSE ** -0.5).astype(jnp.bfloat16)
    w_gate = (jax.random.normal(keys_all[9], (PP, EXPERTS, HIDDEN, FF_EXPERT), jnp.float32) * HIDDEN ** -0.5).astype(jnp.bfloat16)
    w_up = (jax.random.normal(keys_all[10], (PP, EXPERTS, HIDDEN, FF_EXPERT), jnp.float32) * HIDDEN ** -0.5).astype(jnp.bfloat16)
    w_down = (jax.random.normal(keys_all[11], (PP, EXPERTS, FF_EXPERT, HIDDEN), jnp.float32) * FF_EXPERT ** -0.5).astype(jnp.bfloat16)
    return {'x_fwd': x_fwd, 'x_bwd': x_bwd, 'dy_bwd': dy_bwd, 'ids_fwd': ids_fwd, 'gate_fwd': gate_fwd, 'ids_bwd': ids_bwd, 'gate_bwd': gate_bwd, 'w_in': w_in, 'w_out': w_out, 'w_gate': w_gate, 'w_up': w_up, 'w_down': w_down}


def rms_norm(rows_in):
    rows_f32 = rows_in.astype(jnp.float32)
    return (rows_f32 * lax.rsqrt(jnp.mean(rows_f32 * rows_f32, axis=-1, keepdims=True) + EPS_NORM)).astype(jnp.bfloat16)


def slot_index(ids_tok):
    src_ids = ids_tok.reshape(EP, ROUTES)
    onehot = (src_ids[:, :, None] == jnp.arange(EXPERTS)[None, None, :]).astype(jnp.int32)
    route_rank = jnp.sum(jnp.cumsum(onehot, axis=1) * onehot, axis=-1) - 1
    slot_flat = (jnp.arange(EP)[:, None] * EXPERTS + src_ids) * CAPACITY + route_rank
    return slot_flat.reshape(EP * ROUTES)


def stage_forward(x_tok, ids_tok, gate_tok, stage_w_in, stage_w_out, gate_w, up_w, down_w):
    norm_in = rms_norm(x_tok)
    pre_act = jnp.dot(norm_in, stage_w_in, preferred_element_type=jnp.float32).astype(jnp.bfloat16)
    hidden = jax.nn.silu(pre_act.astype(jnp.float32)).astype(jnp.bfloat16)
    mid_res = (x_tok.astype(jnp.float32) + jnp.dot(hidden, stage_w_out, preferred_element_type=jnp.float32)).astype(jnp.bfloat16)
    norm_x = rms_norm(mid_res)
    slot_flat = slot_index(ids_tok)
    norm_rep = jnp.broadcast_to(norm_x.astype(jnp.float32)[:, None, :], (EP * TOKENS, TOP, HIDDEN)).astype(jnp.bfloat16).reshape(EP * ROUTES, HIDDEN)
    row_buf = jnp.zeros((EP * EXPERTS * CAPACITY, HIDDEN), jnp.bfloat16).at[slot_flat].set(norm_rep)
    rows_f32 = row_buf.reshape(EP, EXPERTS, CAPACITY, HIDDEN).astype(jnp.float32)
    gate_pre = jnp.einsum('sech,ehf->secf', rows_f32, gate_w.astype(jnp.float32)).astype(jnp.bfloat16)
    up_pre = jnp.einsum('sech,ehf->secf', rows_f32, up_w.astype(jnp.float32)).astype(jnp.bfloat16)
    act_val = (jax.nn.silu(gate_pre.astype(jnp.float32)) * up_pre.astype(jnp.float32)).astype(jnp.bfloat16)
    expert_out = jnp.einsum('secf,efh->sech', act_val.astype(jnp.float32), down_w.astype(jnp.float32)).astype(jnp.bfloat16)
    routed = expert_out.reshape(EP * EXPERTS * CAPACITY, HIDDEN)[slot_flat].reshape(EP * TOKENS, TOP, HIDDEN)
    mix_sum = jnp.einsum('nk,nkh->nh', gate_tok.astype(jnp.float32), routed.astype(jnp.float32))
    return (mid_res.astype(jnp.float32) + mix_sum).astype(jnp.bfloat16)


def reference(x_fwd, x_bwd, dy_bwd, ids_fwd, gate_fwd, ids_bwd, gate_bwd, w_in, w_out, w_gate, w_up, w_down):
    def one_stage(stage_args):
        fwd_x, bwd_x, bwd_dy, fwd_ids, fwd_gate, bwd_ids, bwd_gate, stage_w_in, stage_w_out, stage_wg, stage_wu, stage_wd = stage_args
        gate_w = stage_wg.astype(jnp.float32)
        up_w = stage_wu.astype(jnp.float32)
        down_w = stage_wd.astype(jnp.float32)
        y_val = stage_forward(fwd_x, fwd_ids, fwd_gate, stage_w_in, stage_w_out, gate_w, up_w, down_w)

        def bwd_map(x_tok, gate_wa, up_wa, down_wa):
            return stage_forward(x_tok, bwd_ids, bwd_gate, stage_w_in, stage_w_out, gate_wa, up_wa, down_wa)

        _, pullback = jax.vjp(bwd_map, bwd_x, gate_w, up_w, down_w)
        dx_val, dw_gate, dw_up, dw_down = pullback(bwd_dy)
        return y_val, dx_val, dw_gate, dw_up, dw_down

    y_all, dx_all, dw_gate, dw_up, dw_down = lax.map(one_stage, (x_fwd, x_bwd, dy_bwd, ids_fwd, gate_fwd, ids_bwd, gate_bwd, w_in, w_out, w_gate, w_up, w_down))
    return jnp.roll(y_all, 1, axis=0), jnp.roll(dx_all, -1, axis=0), dw_gate, dw_up, dw_down
```

```python
import functools

import jax
import jax.numpy as jnp
from jax import lax
from jax.experimental import pallas as pl
from jax.experimental.pallas import tpu as pltpu
from jax.sharding import PartitionSpec as P

EPS_NORM = 1e-6
SUB = 256
PER_TILE = 2
WIN = 512
CHUNK = 256
E_RUN = 4

f32 = jnp.float32
bf16 = jnp.bfloat16
i32 = jnp.int32


def rms_norm(rows_in):
    rows_f32 = rows_in.astype(f32)
    return (rows_f32 * lax.rsqrt(jnp.mean(rows_f32 * rows_f32, axis=-1, keepdims=True) + EPS_NORM)).astype(bf16)


def dense_act(pre_act):
    return jax.nn.silu(pre_act.astype(f32)).astype(bf16)


def dot_nn(a, b):
    return lax.dot_general(a, b, (((1,), (0,)), ((), ())), preferred_element_type=f32)


def dot_nt(a, b):
    return lax.dot_general(a, b, (((1,), (1,)), ((), ())), preferred_element_type=f32)


def dot_tn(a, b):
    return lax.dot_general(a, b, (((0,), (0,)), ((), ())), preferred_element_type=f32)


def expert_kernel(bwd, carry, n_sub, *refs):
    refs = list(refs)

    def take(n):
        out = refs[:n]
        del refs[:n]
        return out

    starts, nwins, ntiles, base_ref, rank_ref, gate_ref = take(6)
    tok_in = take(2)
    dy_in = take(2) if bwd else []
    w_own = take(3)
    w_mate = take(3)
    dw_in = take(6) if carry else []
    p_out = take(2)
    dw_out = take(6) if bwd else []
    tok, acc, wg_buf, wu_buf, wd_buf, x_acc = take(6)
    if bwd:
        dyt, d_acc, xt, dt, dg_all, du_all, dwg_buf, dwu_buf, dwd_buf = take(9)
        tok_sem, w_sem, in_sem, out_sem = take(4)
    else:
        (act_all,) = take(1)
        tok_sem, w_sem = take(2)
    half = tok_in[0].shape[0]
    n_tok = 2 * half
    width = tok.shape[1]
    ff = wg_buf.shape[2]
    base = base_ref[0]

    loads = []
    for i, (src, dst) in enumerate([(tok_in, tok)] + ([(dy_in, dyt)] if bwd else [])):
        for j in range(2):
            loads.append(pltpu.make_async_copy(src[j], dst.at[pl.ds(j * half, half), :], tok_sem.at[i, j]))
    for c in loads:
        c.start()

    def w_copies(srcs, idx, slot):
        return [pltpu.make_async_copy(s.at[idx], b.at[slot], w_sem.at[slot, k])
                for k, (s, b) in enumerate(zip(srcs, (wg_buf, wu_buf, wd_buf)))]

    def w_start(e, slot):
        @pl.when(e < 2)
        def _():
            for c in w_copies(w_own, base + e, slot):
                c.start()

        @pl.when(e >= 2)
        def _():
            for c in w_copies(w_mate, base + e - 2, slot):
                c.start()

    def dw_copies(refs6, e, slot, sem, inward):
        bufs = (dwg_buf, dwu_buf, dwd_buf)

        def go(refs3, idx, what):
            for k in range(3):
                hbm, buf = refs3[k].at[idx], bufs[k].at[slot]
                c = pltpu.make_async_copy(hbm, buf, sem.at[slot, k]) if inward else pltpu.make_async_copy(buf, hbm, sem.at[slot, k])
                getattr(c, what)()

        def start():
            @pl.when(e < 2)
            def _():
                go(refs6[:3], base + e, 'start')

            @pl.when(e >= 2)
            def _():
                go(refs6[3:], e - 2, 'start')

        def wait():
            go(refs6[3:], 0, 'wait')

        return start, wait

    w_start(0, 0)
    if carry:
        dw_copies(dw_in, 0, 0, in_sem, True)[0]()
    acc[...] = jnp.zeros_like(acc)
    for c in loads:
        c.wait()

    def window(e, st, k):
        so = starts[e * n_sub + st] + k * WIN
        s = pl.multiple_of(jnp.minimum(so, n_tok - WIN), 128)
        rk = rank_ref[e, :, pl.ds(s, WIN)]
        lane = lax.broadcasted_iota(i32, (1, WIN), 1) + s
        rk = jnp.where(lane >= so, rk, -1) - st * SUB
        mask = lax.broadcasted_iota(i32, (SUB, WIN), 0) == rk
        return s, mask

    def ones(mask):
        return jnp.where(mask, 1.0, 0.0).astype(bf16)

    def gated(mask, e, s):
        return jnp.where(mask, gate_ref[e, :, pl.ds(s, WIN)], 0.0).astype(bf16)

    def expert(e, _):
        slot = lax.rem(e, 2)
        for c in w_copies(w_own, 0, slot):
            c.wait()

        @pl.when(e < E_RUN - 1)
        def _():
            w_start(e + 1, 1 - slot)

        wg, wu, wd = wg_buf.at[slot], wu_buf.at[slot], wd_buf.at[slot]
        if bwd:
            if carry:
                dw_copies(dw_in, e, slot, in_sem, True)[1]()
            else:
                for b in (dwg_buf, dwu_buf, dwd_buf):
                    b[slot] = jnp.zeros(b.shape[1:], f32)
            dwg, dwu, dwd = dwg_buf.at[slot], dwu_buf.at[slot], dwd_buf.at[slot]

        def tile(t, _):
            for h in range(PER_TILE):
                st = t * PER_TILE + h
                rows = pl.ds(h * SUB, SUB)
                s, mask = window(e, st, 0)
                x_acc[rows, :] = dot_nn(ones(mask), tok[pl.ds(s, WIN), :])
                if bwd:
                    d_acc[rows, :] = dot_nn(gated(mask, e, s), dyt[pl.ds(s, WIN), :])
            for h in range(PER_TILE):
                st = t * PER_TILE + h
                rows = pl.ds(h * SUB, SUB)

                @pl.loop(1, nwins[e * n_sub + st])
                def _(k):
                    s, mask = window(e, st, k)
                    x_acc[rows, :] += dot_nn(ones(mask), tok[pl.ds(s, WIN), :])
                    if bwd:
                        d_acc[rows, :] += dot_nn(gated(mask, e, s), dyt[pl.ds(s, WIN), :])

            x = x_acc[...].astype(bf16)
            if bwd:
                d = d_acc[...].astype(bf16)
                xt[...] = x.T
                dt[...] = d.T
            for c in range(0, ff, CHUNK):
                cols = pl.ds(c, CHUNK)
                gp = dot_nn(x, wg[:, cols]).astype(bf16).astype(f32)
                up = dot_nn(x, wu[:, cols]).astype(bf16).astype(f32)
                sig = 1.0 / (1.0 + jnp.exp(-gp))
                silu = gp * sig
                if not bwd:
                    act_all[:, cols] = (silu * up).astype(bf16)
                    continue
                da = dot_nt(d, wd[cols, :]).astype(bf16).astype(f32)
                act = (silu * up).astype(bf16)
                du = (da * silu).astype(bf16)
                dg = (da * up * (sig + silu * (1.0 - sig))).astype(bf16)
                dg_all[:, cols] = dg
                du_all[:, cols] = du
                dwd[:, cols] += dot_nn(dt[...], act)
                dwg[:, cols] += dot_nn(xt[...], dg)
                dwu[:, cols] += dot_nn(xt[...], du)
            if bwd:
                out = (dot_nt(dg_all[...], wg[...]) + dot_nt(du_all[...], wu[...])).astype(bf16)
            else:
                out = dot_nn(act_all[...], wd[...]).astype(bf16)

            def put(st, k, part):
                s, mask = window(e, st, k)
                sel = ones(mask) if bwd else gated(mask, e, s)
                acc[pl.ds(s, WIN), :] += dot_tn(sel, part)

            for h in range(PER_TILE):
                put(t * PER_TILE + h, 0, out[h * SUB:(h + 1) * SUB, :])
            x_acc[...] = out.astype(f32)
            for h in range(PER_TILE):
                st = t * PER_TILE + h

                @pl.loop(1, nwins[e * n_sub + st])
                def _(k):
                    put(st, k, x_acc[h * SUB:(h + 1) * SUB, :].astype(bf16))

            if bwd:
                @pl.when(t == 0)
                def _():
                    @pl.when(e >= 1)
                    def _():
                        dw_copies(dw_out, e - 1, 1 - slot, out_sem, False)[1]()

                    if carry:
                        @pl.when(e < E_RUN - 1)
                        def _():
                            dw_copies(dw_in, e + 1, 1 - slot, in_sem, True)[0]()
            return 0

        lax.fori_loop(0, ntiles[e], tile, 0)
        if bwd:
            dw_copies(dw_out, e, slot, out_sem, False)[0]()
        return 0

    lax.fori_loop(0, E_RUN, expert, 0)
    outs = [pltpu.make_async_copy(acc.at[pl.ds(j * half, half), :], p_out[j], tok_sem.at[0, j]) for j in range(2)]
    for c in outs:
        c.start()
    if bwd:
        dw_copies(dw_out, E_RUN - 1, (E_RUN - 1) % 2, out_sem, False)[1]()
    for c in outs:
        c.wait()


def run_experts(meta, toks, dys, w_own, w_mate, dw_prev):
    starts, nwins, ntiles, base, rank, gate = meta
    bwd = dys is not None
    carry = dw_prev is not None
    half, width = toks[0].shape
    e_loc, _, ff = w_own[0].shape
    smem = pl.BlockSpec(memory_space=pltpu.SMEM)
    vmem = pl.BlockSpec(memory_space=pltpu.VMEM)
    hbm = pl.BlockSpec(memory_space=pl.ANY)
    args = [starts, nwins, ntiles, base, rank, gate, *toks]
    if bwd:
        args += [*dys]
    args += [*w_own, *w_mate]
    if carry:
        args += [*dw_prev]
    in_specs = [smem] * 4 + [vmem] * 2 + [hbm] * (len(args) - 6)
    out_shape = [jax.ShapeDtypeStruct((half, width), f32)] * 2
    if bwd:
        shape_w = (width, ff)
        for n in (e_loc, 2):
            out_shape += [jax.ShapeDtypeStruct((n, *shape_w), f32)] * 3
    rows = SUB * PER_TILE
    scratch = [
        pltpu.VMEM((2 * half, width), bf16),
        pltpu.VMEM((2 * half, width), f32),
        pltpu.VMEM((2, width, ff), bf16),
        pltpu.VMEM((2, width, ff), bf16),
        pltpu.VMEM((2, ff, width), bf16),
        pltpu.VMEM((rows, width), f32),
    ]
    if bwd:
        scratch += [
            pltpu.VMEM((2 * half, width), bf16),
            pltpu.VMEM((rows, width), f32),
            pltpu.VMEM((width, rows), bf16),
            pltpu.VMEM((width, rows), bf16),
            pltpu.VMEM((rows, ff), bf16),
            pltpu.VMEM((rows, ff), bf16),
            pltpu.VMEM((2, width, ff), f32),
            pltpu.VMEM((2, width, ff), f32),
            pltpu.VMEM((2, width, ff), f32),
            pltpu.SemaphoreType.DMA((2, 2)),
            pltpu.SemaphoreType.DMA((2, 3)),
            pltpu.SemaphoreType.DMA((2, 3)),
            pltpu.SemaphoreType.DMA((2, 3)),
        ]
    else:
        scratch += [
            pltpu.VMEM((rows, ff), bf16),
            pltpu.SemaphoreType.DMA((2, 2)),
            pltpu.SemaphoreType.DMA((2, 3)),
        ]
    n_sub = starts.shape[0] // E_RUN
    flops = (8 if bwd else 3) * 2 * 3584 * 2 * width * ff
    return pl.pallas_call(
        functools.partial(expert_kernel, bwd, carry, n_sub),
        out_shape=out_shape,
        in_specs=in_specs,
        out_specs=[hbm] * len(out_shape),
        scratch_shapes=scratch,
        compiler_params=pltpu.CompilerParams(vmem_limit_bytes=60 * 1024 * 1024),
        cost_estimate=pl.CostEstimate(flops=flops, bytes_accessed=60_000_000, transcendentals=0),
        name='experts_bwd' if bwd else 'experts_fwd',
    )(*args)


def solution(mesh):
    n_ep = mesh.shape['ep']
    n_pp = mesh.shape['pp']
    fwd_perm = [(i, (i + 1) % n_pp) for i in range(n_pp)]
    bwd_perm = [(i, (i - 1) % n_pp) for i in range(n_pp)]

    def to_mate(v):
        return lax.ppermute(v, 'ep', [(i, i ^ 1) for i in range(n_ep)])

    def to_cross(v):
        return lax.ppermute(v, 'ep', [(i, i ^ 2) for i in range(n_ep)])

    def device_fn(x_fwd, x_bwd, dy_bwd, ids_fwd, gate_fwd, ids_bwd, gate_bwd, w_in, w_out, w_gate, w_up, w_down):
        fwd_x, bwd_x, bwd_dy = x_fwd[0], x_bwd[0], dy_bwd[0]
        stage_w_in, stage_w_out = w_in[0], w_out[0]
        w_own = (w_gate[0], w_up[0], w_down[0])
        n_tok, width = fwd_x.shape
        top_k = ids_fwd.shape[2]
        e_loc = w_own[0].shape[0]
        n_exp = e_loc * n_ep
        cap = 3 * n_tok * top_k // n_exp
        me = lax.axis_index('ep')
        core = lax.rem(me, 2)
        base = 2 * core
        n_sub = 2 * cap // SUB

        def gather_pair(v):
            far = to_cross(v)
            return (v, to_mate(v)), (far, to_mate(far))

        dy_near, dy_far = gather_pair(bwd_dy)
        w_mate = tuple(to_mate(w) for w in w_own)

        fields = [ids_fwd[0].astype(f32).T, gate_fwd[0].astype(f32).T, ids_bwd[0].astype(f32).T, gate_bwd[0].astype(f32).T]
        table = lax.all_gather(jnp.concatenate(fields), 'ep')
        table = jnp.take(table, jnp.stack([me, me ^ 1, me ^ 2, me ^ 3]), axis=0)
        mine = e_loc * me + base
        mates = e_loc * (me ^ 1) + base
        run_ids = jnp.stack([mine, mine + 1, mates, mates + 1]).astype(f32)
        base_arr = base.reshape(1).astype(i32)
        tri = jnp.triu(jnp.ones((128, 128), bf16))

        def routing(off):
            ids = table[:, off:off + top_k]
            gates = table[:, off + top_k:off + 2 * top_k]
            match = ids[None] == run_ids[:, None, None, None]
            hit = jnp.any(match, axis=2)
            gate = jnp.sum(jnp.where(match, gates[None], 0.0), axis=2)
            n2 = 2 * n_tok
            hit = hit.reshape(E_RUN, 2, n2 // 128, 128)
            within = jnp.dot(hit.astype(bf16), tri, preferred_element_type=f32)
            tot = within[..., -1]
            blk = jnp.arange(n2 // 128)
            before = jnp.sum(jnp.where(blk[:, None] < blk[None, :], tot[..., :, None], 0.0), axis=2)
            incl = (within + before[..., None]).astype(i32)
            rank = jnp.where(hit, incl - 1, -1).reshape(E_RUN, 2, n2)
            incl = incl.reshape(E_RUN, 2, n2)
            cnt = incl[..., -1]
            first = jnp.arange(n_sub, dtype=i32) * SUB
            last = jnp.minimum(first + SUB, cnt[..., None]) - 1
            start = jnp.sum((incl[:, :, None, :] <= first[None, None, :, None]).astype(i32), axis=-1)
            end = jnp.sum((incl[:, :, None, :] <= last[..., None]).astype(i32), axis=-1) + 1
            start = jnp.minimum(start, n2 - 1) // 128 * 128
            nwin = jnp.maximum((end - start + WIN - 1) // WIN, 1)
            rows = SUB * PER_TILE
            ntile = jnp.maximum((cnt + rows - 1) // rows, 1)
            gate = gate.reshape(E_RUN, 2, n2)
            return [(start[:, i].reshape(-1), nwin[:, i].reshape(-1), ntile[:, i], base_arr,
                     rank[:, i][:, None, :], gate[:, i][:, None, :]) for i in range(2)]

        def dense_fwd(x_tok):
            norm_in = rms_norm(x_tok)
            pre_act = jnp.dot(norm_in, stage_w_in, preferred_element_type=f32).astype(bf16)
            mid_res = (x_tok.astype(f32) + jnp.dot(dense_act(pre_act), stage_w_out, preferred_element_type=f32)).astype(bf16)
            return pre_act, mid_res

        def combine_far(parts):
            return to_cross(parts[0] + to_mate(parts[1]))

        _, mid_f = dense_fwd(fwd_x)
        norm_f = rms_norm(mid_f)
        near_f, far_f = gather_pair(norm_f)
        pre_b, mid_b = dense_fwd(bwd_x)
        norm_b, norm_back = jax.vjp(rms_norm, mid_b)
        near_b, far_b = gather_pair(norm_b)
        meta_near_f, meta_far_f = routing(0)
        meta_near_b, meta_far_b = routing(2 * top_k)

        pf_near = run_experts(meta_near_f, near_f, None, w_own, w_mate, None)
        pf_far = run_experts(meta_far_f, far_f, None, w_own, w_mate, None)
        ret_f = combine_far(pf_far)
        pb_far = run_experts(meta_far_b, far_b, dy_far, w_own, w_mate, None)
        ret_b = combine_far(pb_far[:2])
        pb_near = run_experts(meta_near_b, near_b, dy_near, w_own, w_mate, pb_far[2:])
        dw_full, dw_mate = pb_near[2:5], pb_near[5:8]

        y_val = (mid_f.astype(f32) + (pf_near[0] + to_mate(pf_near[1]) + ret_f)).astype(bf16)
        y_next = lax.ppermute(y_val, 'pp', fwd_perm)

        d_norm = (pb_near[0] + to_mate(pb_near[1]) + ret_b).astype(bf16)
        d_mid = bwd_dy + norm_back(d_norm)[0]
        d_hidden = jnp.einsum('th,fh->tf', d_mid, stage_w_out, preferred_element_type=f32).astype(bf16)
        _, dense_back = jax.vjp(dense_act, pre_b)
        d_pre = dense_back(d_hidden)[0]
        d_norm_in = jnp.einsum('tf,hf->th', d_pre, stage_w_in, preferred_element_type=f32).astype(bf16)
        _, norm_in_back = jax.vjp(rms_norm, bwd_x)
        dx_val = d_mid + norm_in_back(d_norm_in)[0]
        dx_prev = lax.ppermute(dx_val, 'pp', bwd_perm)

        back = [to_mate(v) for v in dw_mate]
        zero = jnp.zeros((), i32)
        dw_gate, dw_up, dw_down_t = [lax.dynamic_update_slice(full, part, (2 - base, zero, zero)) for full, part in zip(dw_full, back)]
        dw_down = jnp.swapaxes(dw_down_t, 1, 2)
        return y_next[None], dx_prev[None], dw_gate[None], dw_up[None], dw_down[None]

    spec_act = P('pp', 'ep', None)
    spec_dense = P('pp', None, None)
    spec_exp = P('pp', 'ep', None, None)
    return jax.shard_map(device_fn, mesh=mesh, in_specs=(spec_act,) * 7 + (spec_dense,) * 2 + (spec_exp,) * 3, out_specs=(spec_act, spec_act, spec_exp, spec_exp, spec_exp), check_vma=False)
```

```python
import functools

import jax
import jax.numpy as jnp
from jax import lax
from jax.experimental import pallas as pl
from jax.experimental.pallas import tpu as pltpu
from jax.sharding import PartitionSpec as P


EPS_NORM = 1e-6
SUB = 256
PER_TILE = 2
WIN = 512
WIN_MORE = 1024
CHUNK = 256
E_RUN = 4

f32 = jnp.float32
bf16 = jnp.bfloat16
i32 = jnp.int32


def rms_norm(rows_in):
    rows_f32 = rows_in.astype(f32)
    return (rows_f32 * lax.rsqrt(jnp.mean(rows_f32 * rows_f32, axis=-1, keepdims=True) + EPS_NORM)).astype(bf16)


def dense_act(pre_act):
    return jax.nn.silu(pre_act.astype(f32)).astype(bf16)


def dot_nn(a, b):
    return lax.dot_general(a, b, (((1,), (0,)), ((), ())), preferred_element_type=f32)


def dot_nt(a, b):
    return lax.dot_general(a, b, (((1,), (1,)), ((), ())), preferred_element_type=f32)


def dot_tn(a, b):
    return lax.dot_general(a, b, (((0,), (0,)), ((), ())), preferred_element_type=f32)


def expert_kernel(bwd, carry, row0, *refs):
    refs = list(refs)

    def take(n):
        out = refs[:n]
        del refs[:n]
        return out

    starts, nwins, ntiles, base_ref, rank_ref, gate_ref = take(6)
    tok_in = take(2)
    dy_in = take(2) if bwd else []
    w_own = take(3)
    w_mate = take(3)
    dw_in = take(6) if carry else []
    p_out = take(2)
    dw_out = take(6) if bwd else []
    tok, acc, wg_buf, wu_buf, wd_buf, x_acc = take(6)
    if bwd:
        dyt, d_acc, xt, dg_all, du_all, dwg_buf, dwu_buf, dwd_buf = take(8)
        tok_sem, w_sem, in_sem, out_sem = take(4)
    else:
        (act_all,) = take(1)
        tok_sem, w_sem = take(2)
    half = tok_in[0].shape[0]
    n_tok = 2 * half
    ff = wg_buf.shape[2]
    base = base_ref[0]

    loads = []
    for i, (src, dst) in enumerate([(tok_in, tok)] + ([(dy_in, dyt)] if bwd else [])):
        for j in range(2):
            loads.append(pltpu.make_async_copy(src[j], dst.at[pl.ds(j * half, half), :], tok_sem.at[i, j]))
    for c in loads:
        c.start()

    def w_copies(srcs, idx, slot):
        return [pltpu.make_async_copy(s.at[idx], b.at[slot], w_sem.at[slot, k])
                for k, (s, b) in enumerate(zip(srcs, (wg_buf, wu_buf, wd_buf)))]

    def w_start(e, slot):
        @pl.when(e < 2)
        def _():
            for c in w_copies(w_own, base + e, slot):
                c.start()

        @pl.when(e >= 2)
        def _():
            for c in w_copies(w_mate, base + e - 2, slot):
                c.start()

    def dw_copies(refs6, e, slot, sem, inward):
        bufs = (dwg_buf, dwu_buf, dwd_buf)

        def go(refs3, idx, what):
            for k in range(3):
                hbm, buf = refs3[k].at[idx], bufs[k].at[slot]
                c = pltpu.make_async_copy(hbm, buf, sem.at[slot, k]) if inward else pltpu.make_async_copy(buf, hbm, sem.at[slot, k])
                getattr(c, what)()

        def start():
            @pl.when(e < 2)
            def _():
                go(refs6[:3], base + e, 'start')

            @pl.when(e >= 2)
            def _():
                go(refs6[3:], e - 2, 'start')

        def wait():
            go(refs6[3:], 0, 'wait')

        return start, wait

    w_start(0, 0)
    if carry:
        dw_copies(dw_in, 0, 0, in_sem, True)[0]()
    acc[...] = jnp.zeros_like(acc)
    for c in loads:
        c.wait()

    def window(e, st, k):
        size = WIN_MORE if k is not None else WIN
        so = starts[row0 + e, st]
        if k is not None:
            so += WIN + (k - 1) * WIN_MORE
        s = pl.multiple_of(jnp.minimum(so, n_tok - size), 128)
        rk = rank_ref[pl.ds(row0 + e, 1), pl.ds(s, size)]
        lane = lax.broadcasted_iota(i32, (1, size), 1) + s
        rk = jnp.where(lane >= so, rk, -1) - st * SUB
        mask = lax.broadcasted_iota(i32, (SUB, size), 0) == rk
        return pl.ds(s, size), mask

    def ones(mask):
        return jnp.where(mask, 1.0, 0.0).astype(bf16)

    def gated(mask, e, win):
        return jnp.where(mask, gate_ref[pl.ds(row0 + e, 1), win], 0.0).astype(bf16)

    def expert(e, _):
        slot = lax.rem(e, 2)
        for c in w_copies(w_own, 0, slot):
            c.wait()

        @pl.when(e < E_RUN - 1)
        def _():
            w_start(e + 1, 1 - slot)

        wg, wu, wd = wg_buf.at[slot], wu_buf.at[slot], wd_buf.at[slot]
        if bwd:
            if carry:
                dw_copies(dw_in, e, slot, in_sem, True)[1]()
            else:
                for b in (dwg_buf, dwu_buf, dwd_buf):
                    b[slot] = jnp.zeros(b.shape[1:], f32)
            dwg, dwu, dwd = dwg_buf.at[slot], dwu_buf.at[slot], dwd_buf.at[slot]

        def tile(t, _):
            for h in range(PER_TILE):
                st = t * PER_TILE + h
                rows = pl.ds(h * SUB, SUB)
                win, mask = window(e, st, None)
                x_acc[rows, :] = dot_nn(ones(mask), tok[win, :])
                if bwd:
                    d_acc[rows, :] = dot_nn(gated(mask, e, win), dyt[win, :])
            for h in range(PER_TILE):
                st = t * PER_TILE + h
                rows = pl.ds(h * SUB, SUB)

                @pl.loop(1, nwins[row0 + e, st])
                def _(k):
                    win, mask = window(e, st, k)
                    x_acc[rows, :] += dot_nn(ones(mask), tok[win, :])
                    if bwd:
                        d_acc[rows, :] += dot_nn(gated(mask, e, win), dyt[win, :])

            x = x_acc[...].astype(bf16)
            if bwd:
                d = d_acc[...].astype(bf16)
                xt[...] = x.T
            for c in range(0, ff, CHUNK):
                cols = pl.ds(c, CHUNK)
                gp = dot_nn(x, wg[:, cols]).astype(bf16).astype(f32)
                up = dot_nn(x, wu[:, cols]).astype(bf16).astype(f32)
                sig = 1.0 / (1.0 + jnp.exp(-gp))
                silu = gp * sig
                if not bwd:
                    act_all[:, cols] = (silu * up).astype(bf16)
                    continue
                da = dot_nt(d, wd[cols, :]).astype(bf16).astype(f32)
                act = (silu * up).astype(bf16)
                du = (da * silu).astype(bf16)
                dg = (da * up * (sig + silu * (1.0 - sig))).astype(bf16)
                dg_all[:, cols] = dg
                du_all[:, cols] = du
                dwd[cols, :] += dot_tn(act, d)
                dwg[:, cols] += dot_nn(xt[...], dg)
                dwu[:, cols] += dot_nn(xt[...], du)
            if bwd:
                out = (dot_nt(dg_all[...], wg[...]) + dot_nt(du_all[...], wu[...])).astype(bf16)
            else:
                out = dot_nn(act_all[...], wd[...]).astype(bf16)

            def put(st, k, part):
                win, mask = window(e, st, k)
                sel = ones(mask) if bwd else gated(mask, e, win)
                acc[win, :] += dot_tn(sel, part)

            for h in range(PER_TILE):
                put(t * PER_TILE + h, None, out[h * SUB:(h + 1) * SUB, :])
            x_acc[...] = out.astype(f32)
            for h in range(PER_TILE):
                st = t * PER_TILE + h

                @pl.loop(1, nwins[row0 + e, st])
                def _(k):
                    put(st, k, x_acc[h * SUB:(h + 1) * SUB, :].astype(bf16))

            if bwd:
                @pl.when(t == 0)
                def _():
                    @pl.when(e >= 1)
                    def _():
                        dw_copies(dw_out, e - 1, 1 - slot, out_sem, False)[1]()

                    if carry:
                        @pl.when(e < E_RUN - 1)
                        def _():
                            dw_copies(dw_in, e + 1, 1 - slot, in_sem, True)[0]()
            return 0

        lax.fori_loop(0, ntiles[row0 + e, 0], tile, 0)
        if bwd:
            dw_copies(dw_out, e, slot, out_sem, False)[0]()
        return 0

    lax.fori_loop(0, E_RUN, expert, 0)
    outs = [pltpu.make_async_copy(acc.at[pl.ds(j * half, half), :], p_out[j], tok_sem.at[0, j]) for j in range(2)]
    for c in outs:
        c.start()
    if bwd:
        dw_copies(dw_out, E_RUN - 1, (E_RUN - 1) % 2, out_sem, False)[1]()
    for c in outs:
        c.wait()


def routing_kernel(n_sub, who_ref, tab_ref, rank_ref, gate_ref, start_ref, nwin_ref, ntile_ref, hit_ref):
    _, fields, n_tok = tab_ref.shape
    top_k = fields // 4
    n2 = 2 * n_tok
    n_blk = n2 // 128
    r_i = lax.broadcasted_iota(i32, (128, 128), 0)
    c_i = lax.broadcasted_iota(i32, (128, 128), 1)
    tri = jnp.where(r_i <= c_i, 1.0, 0.0).astype(bf16)
    full = jnp.ones((128, 128), bf16)
    lane = lax.broadcasted_iota(i32, (2 * E_RUN, 128), 1)
    for mb in range(2):
        for q in range(4):
            part = tab_ref[who_ref[q], pl.ds(mb * 2 * top_k, 2 * top_k), :]
            ids, gates = part[:top_k], part[top_k:]
            cols = pl.ds((q % 2) * n_tok, n_tok)
            for e in range(E_RUN):
                match = ids == who_ref[4 + e].astype(f32)
                row = (q // 2) * E_RUN + e
                hit_ref[row:row + 1, cols] = jnp.sum(jnp.where(match, 1.0, 0.0), axis=0, keepdims=True)
                gate_ref[mb, row:row + 1, cols] = jnp.sum(jnp.where(match, gates, 0.0), axis=0, keepdims=True)
        hits = [hit_ref[:, b * 128:(b + 1) * 128] for b in range(n_blk)]
        stacked = jnp.concatenate(hits, axis=0).astype(bf16)
        within = dot_nn(stacked, tri)
        totals = dot_nn(stacked, full)
        carry = jnp.zeros((2 * E_RUN, 128), f32)
        incl = []
        for b in range(n_blk):
            rows = slice(b * 2 * E_RUN, (b + 1) * 2 * E_RUN)
            v = (within[rows] + carry).astype(i32)
            rank_ref[mb, :, b * 128:(b + 1) * 128] = jnp.where(hits[b] > 0.5, v - 1, -1)
            incl.append(v)
            carry = carry + totals[rows]
        cnt = carry.astype(i32)

        def tokens_upto(limit):
            tot = jnp.zeros((2 * E_RUN, 128), f32)
            for v in incl:
                tot = tot + jnp.where(v <= limit, 1.0, 0.0)
            return jnp.sum(tot, axis=1, keepdims=True).astype(i32)

        start = jnp.zeros((2 * E_RUN, 128), i32)
        nwin = jnp.ones((2 * E_RUN, 128), i32)
        for j in range(n_sub):
            lo = jnp.minimum(tokens_upto(j * SUB), n2 - 1) // 128 * 128
            hi = tokens_upto(jnp.minimum((j + 1) * SUB, cnt) - 1) + 1
            n = jnp.maximum((hi - lo - WIN + WIN_MORE - 1) // WIN_MORE, 0) + 1
            start = jnp.where(lane == j, lo, start)
            nwin = jnp.where(lane == j, n, nwin)
        start_ref[mb] = start
        nwin_ref[mb] = nwin
        tile_rows = SUB * PER_TILE
        ntile_ref[mb] = jnp.maximum((cnt + tile_rows - 1) // tile_rows, 1)


def run_routing(who, table, n_sub):
    _, _, n_tok = table.shape
    rows = 2 * E_RUN
    wide = (2, rows, 2 * n_tok)
    small = jax.ShapeDtypeStruct((2, rows, 128), i32)
    vmem = pl.BlockSpec(memory_space=pltpu.VMEM)
    return pl.pallas_call(
        functools.partial(routing_kernel, n_sub),
        out_shape=[jax.ShapeDtypeStruct(wide, i32), jax.ShapeDtypeStruct(wide, f32), small, small, small],
        in_specs=[pl.BlockSpec(memory_space=pltpu.SMEM), vmem],
        out_specs=[vmem] * 5,
        scratch_shapes=[pltpu.VMEM((rows, 2 * n_tok), f32)],
        name='routing',
    )(who, table)


def run_experts(meta, far, toks, dys, w_own, w_mate, dw_prev):
    starts, nwins, ntiles, base, rank, gate = meta
    bwd = dys is not None
    carry = dw_prev is not None
    half, width = toks[0].shape
    e_loc, _, ff = w_own[0].shape
    smem = pl.BlockSpec(memory_space=pltpu.SMEM)
    vmem = pl.BlockSpec(memory_space=pltpu.VMEM)
    hbm = pl.BlockSpec(memory_space=pl.ANY)
    args = [starts, nwins, ntiles, base, rank, gate, *toks]
    if bwd:
        args += [*dys]
    args += [*w_own, *w_mate]
    if carry:
        args += [*dw_prev]
    in_specs = [smem] * 4 + [vmem] * 2 + [hbm] * (len(args) - 6)
    out_shape = [jax.ShapeDtypeStruct((half, width), f32)] * 2
    if bwd:
        for n in (e_loc, 2):
            out_shape += [jax.ShapeDtypeStruct((n, *w.shape[1:]), f32) for w in w_own]
    rows = SUB * PER_TILE
    scratch = [
        pltpu.VMEM((2 * half, width), bf16),
        pltpu.VMEM((2 * half, width), f32),
        pltpu.VMEM((2, width, ff), bf16),
        pltpu.VMEM((2, width, ff), bf16),
        pltpu.VMEM((2, ff, width), bf16),
        pltpu.VMEM((rows, width), f32),
    ]
    if bwd:
        scratch += [
            pltpu.VMEM((2 * half, width), bf16),
            pltpu.VMEM((rows, width), f32),
            pltpu.VMEM((width, rows), bf16),
            pltpu.VMEM((rows, ff), bf16),
            pltpu.VMEM((rows, ff), bf16),
            pltpu.VMEM((2, width, ff), f32),
            pltpu.VMEM((2, width, ff), f32),
            pltpu.VMEM((2, ff, width), f32),
            pltpu.SemaphoreType.DMA((2, 2)),
            pltpu.SemaphoreType.DMA((2, 3)),
            pltpu.SemaphoreType.DMA((2, 3)),
            pltpu.SemaphoreType.DMA((2, 3)),
        ]
    else:
        scratch += [
            pltpu.VMEM((rows, ff), bf16),
            pltpu.SemaphoreType.DMA((2, 2)),
            pltpu.SemaphoreType.DMA((2, 3)),
        ]
    flops = (8 if bwd else 3) * 2 * 3584 * 2 * width * ff
    return pl.pallas_call(
        functools.partial(expert_kernel, bwd, carry, E_RUN if far else 0),
        out_shape=out_shape,
        in_specs=in_specs,
        out_specs=[hbm] * len(out_shape),
        scratch_shapes=scratch,
        compiler_params=pltpu.CompilerParams(vmem_limit_bytes=60 * 1024 * 1024),
        cost_estimate=pl.CostEstimate(flops=flops, bytes_accessed=60_000_000, transcendentals=0),
        name='experts_bwd' if bwd else 'experts_fwd',
    )(*args)


def solution(mesh):
    n_ep = mesh.shape['ep']
    n_pp = mesh.shape['pp']
    fwd_perm = [(i, (i + 1) % n_pp) for i in range(n_pp)]
    bwd_perm = [(i, (i - 1) % n_pp) for i in range(n_pp)]

    def to_mate(v):
        return lax.ppermute(v, 'ep', [(i, i ^ 1) for i in range(n_ep)])

    def to_cross(v):
        return lax.ppermute(v, 'ep', [(i, i ^ 2) for i in range(n_ep)])

    def device_fn(x_fwd, x_bwd, dy_bwd, ids_fwd, gate_fwd, ids_bwd, gate_bwd, w_in, w_out, w_gate, w_up, w_down):
        fwd_x, bwd_x, bwd_dy = x_fwd[0], x_bwd[0], dy_bwd[0]
        stage_w_in, stage_w_out = w_in[0], w_out[0]
        w_own = (w_gate[0], w_up[0], w_down[0])
        n_tok, _ = fwd_x.shape
        top_k = ids_fwd.shape[2]
        e_loc = w_own[0].shape[0]
        n_exp = e_loc * n_ep
        cap = 3 * n_tok * top_k // n_exp
        me = lax.axis_index('ep')
        core = lax.rem(me, 2)
        base = 2 * core
        n_sub = 2 * cap // SUB

        def gather_pair(v):
            far = to_cross(v)
            return (v, to_mate(v)), (far, to_mate(far))

        fields = [ids_fwd[0].astype(f32).T, gate_fwd[0].astype(f32).T, ids_bwd[0].astype(f32).T, gate_bwd[0].astype(f32).T]
        table = lax.all_gather(jnp.concatenate(fields), 'ep')
        mine = e_loc * me + base
        mates = e_loc * (me ^ 1) + base
        who = jnp.stack([me, me ^ 1, me ^ 2, me ^ 3, mine, mine + 1, mates, mates + 1]).astype(i32)
        base_arr = base.reshape(1).astype(i32)
        ranks, gates, starts, nwins, ntiles = run_routing(who, table, n_sub)
        meta_f, meta_b = [(starts[m], nwins[m], ntiles[m], base_arr, ranks[m], gates[m]) for m in range(2)]

        dy_send, w_send = lax.optimization_barrier((bwd_dy, w_own, table))[:2]
        far_dy = to_cross(dy_send)
        dy_near, dy_far = (bwd_dy, to_mate(dy_send)), (far_dy, to_mate(far_dy))
        w_mate = tuple(to_mate(w) for w in w_send)

        def dense_fwd(x_tok):
            norm_in = rms_norm(x_tok)
            pre_act = jnp.dot(norm_in, stage_w_in, preferred_element_type=f32).astype(bf16)
            mid_res = (x_tok.astype(f32) + jnp.dot(dense_act(pre_act), stage_w_out, preferred_element_type=f32)).astype(bf16)
            return pre_act, mid_res

        def combine(parts):
            return parts[0] + to_mate(parts[1])

        _, mid_f = dense_fwd(fwd_x)
        norm_f = rms_norm(mid_f)
        near_f, far_f = gather_pair(norm_f)
        pre_b, mid_b = dense_fwd(bwd_x)
        norm_b, norm_back = jax.vjp(rms_norm, mid_b)
        near_b, far_b = gather_pair(norm_b)

        pf_near = run_experts(meta_f, False, near_f, None, w_own, w_mate, None)
        pf_far = run_experts(meta_f, True, far_f, None, w_own, w_mate, None)
        ret_f = to_cross(combine(pf_far))
        pb_far = run_experts(meta_b, True, far_b, dy_far, w_own, w_mate, None)
        ret_b = to_cross(combine(pb_far[:2]))
        pb_near = run_experts(meta_b, False, near_b, dy_near, w_own, w_mate, pb_far[2:])
        dw_full, dw_mate = pb_near[2:5], pb_near[5:8]

        y_val = (mid_f.astype(f32) + (combine(pf_near) + ret_f)).astype(bf16)
        y_next = lax.ppermute(y_val, 'pp', fwd_perm)

        d_norm = (combine(pb_near) + ret_b).astype(bf16)
        d_mid = bwd_dy + norm_back(d_norm)[0]
        d_hidden = jnp.einsum('th,fh->tf', d_mid, stage_w_out, preferred_element_type=f32).astype(bf16)
        _, dense_back = jax.vjp(dense_act, pre_b)
        d_pre = dense_back(d_hidden)[0]
        d_norm_in = jnp.einsum('tf,hf->th', d_pre, stage_w_in, preferred_element_type=f32).astype(bf16)
        _, norm_in_back = jax.vjp(rms_norm, bwd_x)
        dx_val = d_mid + norm_in_back(d_norm_in)[0]
        dx_prev = lax.ppermute(dx_val, 'pp', bwd_perm)

        back = [to_mate(v) for v in dw_mate]
        zero = jnp.zeros((), i32)
        dw_gate, dw_up, dw_down = [lax.dynamic_update_slice(full, part, (2 - base, zero, zero)) for full, part in zip(dw_full, back)]
        return y_next[None], dx_prev[None], dw_gate[None], dw_up[None], dw_down[None]

    spec_act = P('pp', 'ep', None)
    spec_dense = P('pp', None, None)
    spec_exp = P('pp', 'ep', None, None)


    return jax.shard_map(device_fn, mesh=mesh, in_specs=(spec_act,) * 7 + (spec_dense,) * 2 + (spec_exp,) * 3, out_specs=(spec_act, spec_act, spec_exp, spec_exp, spec_exp), check_vma=False)
```

```python
import functools

import jax
import jax.numpy as jnp
from jax import lax
from jax.experimental import pallas as pl
from jax.experimental.pallas import tpu as pltpu
from jax.sharding import PartitionSpec as P


EPS_NORM = 1e-6
SUB = 128
TILE_SUBS = (3, 4)
WIN = 256
WIN_MORE = 768
ALIGN = 64
CHUNK = 256
DW_SLOTS = 3
TAIL = 4
DENSE_ROWS = 512
E_RUN = 4

f32 = jnp.float32
bf16 = jnp.bfloat16
i32 = jnp.int32


def dot_nn(a, b):
    return lax.dot_general(a, b, (((1,), (0,)), ((), ())), preferred_element_type=f32)


def dot_nt(a, b):
    return lax.dot_general(a, b, (((1,), (1,)), ((), ())), preferred_element_type=f32)


def dot_tn(a, b):
    return lax.dot_general(a, b, (((0,), (0,)), ((), ())), preferred_element_type=f32)


def expert_kernel(bwd, carry, row0, *refs):
    refs = list(refs)

    def take(n):
        out = refs[:n]
        del refs[:n]
        return out

    starts, nwins, ntiles, base_ref, rank_ref, gate_ref = take(6)
    tok_in = take(2)
    dy_in = take(2) if bwd else []
    mb = int(bwd)
    per_tile = TILE_SUBS[mb]
    w_own = take(3)
    w_mate = take(3)
    dw_in = take(6) if carry else []
    p_out = take(2)
    dw_out = take(6) if bwd else []
    tok, acc, wg_buf, wu_buf, wd_buf, x_acc, out_all = take(7)
    if bwd:
        dyt, d_acc, xt, dg_all, du_all, dwg_buf, dwu_buf, dwd_buf = take(8)
        tok_sem, w_sem, in_sem, out_sem = take(4)
    else:
        (act_all,) = take(1)
        tok_sem, w_sem = take(2)
    half = tok_in[0].shape[0]
    n_tok = 2 * half
    ff = wg_buf.shape[2]
    base = base_ref[0]

    loads = []
    for i, (src, dst) in enumerate([(tok_in, tok)] + ([(dy_in, dyt)] if bwd else [])):
        for j in range(2):
            loads.append(pltpu.make_async_copy(src[j], dst.at[pl.ds(j * half, half), :], tok_sem.at[i, j]))
    for c in loads:
        c.start()

    def w_copies(srcs, idx, slot):
        return [pltpu.make_async_copy(s.at[idx], b.at[slot], w_sem.at[slot, k])
                for k, (s, b) in enumerate(zip(srcs, (wg_buf, wu_buf, wd_buf)))]

    def w_start(e, slot):
        @pl.when(e < 2)
        def _():
            for c in w_copies(w_own, base + e, slot):
                c.start()

        @pl.when(e >= 2)
        def _():
            for c in w_copies(w_mate, base + e - 2, slot):
                c.start()

    def dw_copies(refs6, e, slot, sem, inward):
        bufs = (dwg_buf, dwu_buf, dwd_buf)

        def go(refs3, idx, what):
            for k in range(3):
                hbm, buf = refs3[k].at[idx], bufs[k].at[slot]
                c = pltpu.make_async_copy(hbm, buf, sem.at[slot, k]) if inward else pltpu.make_async_copy(buf, hbm, sem.at[slot, k])
                getattr(c, what)()

        def start():
            @pl.when(e < 2)
            def _():
                go(refs6[:3], base + e, 'start')

            @pl.when(e >= 2)
            def _():
                go(refs6[3:], e - 2, 'start')

        def wait():
            go(refs6[3:], 0, 'wait')

        return start, wait

    w_start(0, 0)
    if carry:
        dw_copies(dw_in, 0, 0, in_sem, True)[0]()
    acc[...] = jnp.zeros_like(acc)
    for c in loads:
        c.wait()

    def window(e, st, k):
        size = WIN_MORE if k is not None else WIN
        so = starts[mb, row0 + e, st]
        if k is not None:
            so += WIN + (k - 1) * WIN_MORE
        s = jnp.minimum(so, n_tok - size)
        shift = lax.rem(s // ALIGN, 2)
        lanes = pl.ds(pl.multiple_of(s - shift * ALIGN, 128), size)
        rk = rank_ref[mb, shift, pl.ds(row0 + e, 1), lanes]
        lane = lax.broadcasted_iota(i32, (1, size), 1) + s
        rk = jnp.where(lane >= so, rk, -1) - st * SUB
        mask = lax.broadcasted_iota(i32, (SUB, size), 0) == rk
        toks = pl.ds(pl.multiple_of(s, ALIGN), size)
        return toks, lambda: jnp.where(mask, 1.0, 0.0).astype(bf16), \
            lambda: jnp.where(mask, gate_ref[mb, shift, pl.ds(row0 + e, 1), lanes], 0.0).astype(bf16)

    def expert(e, _):
        slot = lax.rem(e, 2)
        for c in w_copies(w_own, 0, slot):
            c.wait()

        @pl.when(e < E_RUN - 1)
        def _():
            w_start(e + 1, 1 - slot)

        wg, wu, wd = wg_buf.at[slot], wu_buf.at[slot], wd_buf.at[slot]
        if bwd:
            d_slot = lax.rem(e, DW_SLOTS)

            @pl.when(e >= 2)
            def _():
                old = e - 2
                dw_copies(dw_out, old, lax.rem(old, DW_SLOTS), out_sem, False)[1]()

            if carry:
                @pl.when(e < E_RUN - 1)
                def _():
                    dw_copies(dw_in, e + 1, lax.rem(e + 1, DW_SLOTS), in_sem, True)[0]()

                dw_copies(dw_in, e, d_slot, in_sem, True)[1]()
            else:
                for b in (dwg_buf, dwu_buf, dwd_buf):
                    b[d_slot] = jnp.zeros(b.shape[1:], f32)
            dwg, dwu, dwd = dwg_buf.at[d_slot], dwu_buf.at[d_slot], dwd_buf.at[d_slot]

        def tile(t, _):
            for h in range(per_tile):
                rows = pl.ds(h * SUB, SUB)
                toks, ones, gated = window(e, t * per_tile + h, None)
                x_acc[rows, :] = dot_nn(ones(), tok[toks, :])
                if bwd:
                    d_acc[rows, :] = dot_nn(gated(), dyt[toks, :])

            @pl.loop(0, per_tile)
            def _(h):
                st = t * per_tile + h
                rows = pl.ds(pl.multiple_of(h * SUB, SUB), SUB)

                @pl.loop(1, nwins[mb, row0 + e, st])
                def _(k):
                    toks, ones, gated = window(e, st, k)
                    x_acc[rows, :] += dot_nn(ones(), tok[toks, :])
                    if bwd:
                        d_acc[rows, :] += dot_nn(gated(), dyt[toks, :])

            x = x_acc[...].astype(bf16)
            if bwd:
                d = d_acc[...].astype(bf16)
                xt[...] = x.T
            for c in range(0, ff, CHUNK):
                cols = pl.ds(c, CHUNK)
                gp = dot_nn(x, wg[:, cols]).astype(bf16).astype(f32)
                up = dot_nn(x, wu[:, cols]).astype(bf16).astype(f32)
                sig = 1.0 / (1.0 + jnp.exp(-gp))
                silu = gp * sig
                if not bwd:
                    act_all[:, cols] = (silu * up).astype(bf16)
                    continue
                da = dot_nt(d, wd[cols, :]).astype(bf16).astype(f32)
                act = (silu * up).astype(bf16)
                du = (da * silu).astype(bf16)
                dg = (da * up * (sig + silu * (1.0 - sig))).astype(bf16)
                dg_all[:, cols] = dg
                du_all[:, cols] = du
                dwd[cols, :] += dot_tn(act, d)
                dwg[:, cols] += dot_nn(xt[...], dg)
                dwu[:, cols] += dot_nn(xt[...], du)
            if bwd:
                out = (dot_nt(dg_all[...], wg[...]) + dot_nt(du_all[...], wu[...])).astype(bf16)
            else:
                out = dot_nn(act_all[...], wd[...]).astype(bf16)

            def put(st, k, part):
                toks, ones, gated = window(e, st, k)
                acc[toks, :] += dot_tn(ones() if bwd else gated(), part)

            out_all[...] = out
            for h in range(per_tile):
                put(t * per_tile + h, None, out[h * SUB:(h + 1) * SUB, :])

            @pl.loop(0, per_tile)
            def _(h):
                st = t * per_tile + h

                @pl.loop(1, nwins[mb, row0 + e, st])
                def _(k):
                    put(st, k, out_all[pl.ds(pl.multiple_of(h * SUB, SUB), SUB), :])

            return 0

        lax.fori_loop(0, ntiles[mb, row0 + e, 0], tile, 0)
        if bwd:
            dw_copies(dw_out, e, d_slot, out_sem, False)[0]()
        return 0

    lax.fori_loop(0, E_RUN, expert, 0)
    outs = [pltpu.make_async_copy(acc.at[pl.ds(j * half, half), :], p_out[j], tok_sem.at[0, j]) for j in range(2)]
    for c in outs:
        c.start()
    if bwd:
        for e in (E_RUN - 2, E_RUN - 1):
            dw_copies(dw_out, e, e % DW_SLOTS, out_sem, False)[1]()
    for c in outs:
        c.wait()


def routing_kernel(n_sub, who_ref, tab0, tab1, tab2, tab3, rank_ref, gate_ref, start_ref, nwin_ref, ntile_ref, hit_ref):
    fields, n_tok = tab0.shape
    top_k = fields // 4
    n2 = 2 * n_tok
    n_blk = n2 // 128
    r_i = lax.broadcasted_iota(i32, (128, 128), 0)
    c_i = lax.broadcasted_iota(i32, (128, 128), 1)
    tri = jnp.where(r_i <= c_i, 1.0, 0.0).astype(bf16)
    full = jnp.ones((128, 128), bf16)
    lane = lax.broadcasted_iota(i32, (2 * E_RUN, 128), 1)
    for mb in range(2):
        for q, tab in enumerate((tab0, tab1, tab2, tab3)):
            part = tab[mb * 2 * top_k:(mb + 1) * 2 * top_k, :]
            ids, gates = part[:top_k], part[top_k:]
            cols = pl.ds((q % 2) * n_tok, n_tok)
            for e in range(E_RUN):
                match = ids == who_ref[e].astype(f32)
                row = (q // 2) * E_RUN + e
                hit_ref[row:row + 1, cols] = jnp.sum(jnp.where(match, 1.0, 0.0), axis=0, keepdims=True)
                gate_ref[mb, 0, row:row + 1, cols] = jnp.sum(jnp.where(match, gates, 0.0), axis=0, keepdims=True)
        hits = [hit_ref[:, b * 128:(b + 1) * 128] for b in range(n_blk)]
        stacked = jnp.concatenate(hits, axis=0).astype(bf16)
        within = dot_nn(stacked, tri)
        totals = dot_nn(stacked, full)
        carry = jnp.zeros((2 * E_RUN, 128), f32)
        incl = []
        for b in range(n_blk):
            rows = slice(b * 2 * E_RUN, (b + 1) * 2 * E_RUN)
            v = (within[rows] + carry).astype(i32)
            rank_ref[mb, 0, :, b * 128:(b + 1) * 128] = jnp.where(hits[b] > 0.5, v - 1, -1)
            incl.append(v)
            carry = carry + totals[rows]
        for ref, fill in ((rank_ref, -1), (gate_ref, 0.0)):
            ref[mb, 1, :, :n2 - 128] = ref[mb, 0, :, ALIGN:n2 - 128 + ALIGN]
            tail = jnp.concatenate([ref[mb, 0, :, n2 - 128:], jnp.full((2 * E_RUN, 128), fill, ref.dtype)], axis=1)
            ref[mb, 1, :, n2 - 128:] = tail[:, ALIGN:128 + ALIGN]
        cnt = carry.astype(i32)

        def tokens_upto(limit):
            tot = jnp.zeros((2 * E_RUN, 128), f32)
            for v in incl:
                tot = tot + jnp.where(v <= limit, 1.0, 0.0)
            return jnp.sum(tot, axis=1, keepdims=True).astype(i32)

        start = jnp.zeros((2 * E_RUN, 128), i32)
        nwin = jnp.ones((2 * E_RUN, 128), i32)
        for j in range(n_sub):
            lo = jnp.minimum(tokens_upto(j * SUB), n2 - 1) // ALIGN * ALIGN
            hi = tokens_upto(jnp.minimum((j + 1) * SUB, cnt) - 1) + 1
            n = jnp.maximum((hi - lo - WIN + WIN_MORE - 1) // WIN_MORE, 0) + 1
            start = jnp.where(lane == j, lo, start)
            nwin = jnp.where(lane == j, n, nwin)
        start_ref[mb] = start
        nwin_ref[mb] = nwin
        tile_rows = SUB * TILE_SUBS[mb]
        ntile_ref[mb] = jnp.maximum((cnt + tile_rows - 1) // tile_rows, 1)


def run_routing(who, tables, n_sub):
    n_tok = tables[0].shape[1]
    rows = 2 * E_RUN
    wide = (2, 2, rows, 2 * n_tok)
    small = jax.ShapeDtypeStruct((2, rows, 128), i32)
    vmem = pl.BlockSpec(memory_space=pltpu.VMEM)
    return pl.pallas_call(
        functools.partial(routing_kernel, n_sub),
        out_shape=[jax.ShapeDtypeStruct(wide, i32), jax.ShapeDtypeStruct(wide, f32), small, small, small],
        in_specs=[pl.BlockSpec(memory_space=pltpu.SMEM)] + [vmem] * 4,
        out_specs=[vmem] * 5,
        scratch_shapes=[pltpu.VMEM((rows, 2 * n_tok), f32)],
        name='routing',
    )(who, *tables)


def sigmoid(v):
    return 1.0 / (1.0 + jnp.exp(-v))


def rms_scale(rows_f32):
    return lax.rsqrt(jnp.mean(rows_f32 * rows_f32, axis=-1, keepdims=True) + EPS_NORM)


def rms_back(rows_f32, cot):
    cot = cot.astype(f32)
    scale = rms_scale(rows_f32)
    proj = jnp.mean(cot * rows_f32, axis=-1, keepdims=True)
    return (scale * cot - rows_f32 * (scale * scale * scale * proj)).astype(bf16)


def dense_kernel(x_ref, w_in, w_out, norm_ref, mid_ref, *pre_ref):
    x = x_ref[...].astype(f32)
    norm_in = (x * rms_scale(x)).astype(bf16)
    pre = dot_nn(norm_in, w_in[...]).astype(bf16)
    if pre_ref:
        pre_ref[0][...] = pre
    pre = pre.astype(f32)
    hid = (pre * sigmoid(pre)).astype(bf16)
    mid = (x + dot_nn(hid, w_out[...])).astype(bf16)
    mid_ref[...] = mid
    mid = mid.astype(f32)
    norm_ref[...] = (mid * rms_scale(mid)).astype(bf16)


def run_dense(x, w_in, w_out, keep_pre):
    n_tok, width = x.shape
    ff = w_in.shape[1]
    row = pl.BlockSpec((DENSE_ROWS, width), lambda i: (i, 0))
    out_shape = [jax.ShapeDtypeStruct(x.shape, bf16)] * 2
    out_specs = [row, row]
    if keep_pre:
        out_shape += [jax.ShapeDtypeStruct((n_tok, ff), bf16)]
        out_specs += [pl.BlockSpec((DENSE_ROWS, ff), lambda i: (i, 0))]
    return pl.pallas_call(
        dense_kernel,
        grid=(n_tok // DENSE_ROWS,),
        out_shape=out_shape,
        in_specs=[row, pl.BlockSpec((width, ff), lambda i: (0, 0)), pl.BlockSpec((ff, width), lambda i: (0, 0))],
        out_specs=out_specs,
        cost_estimate=pl.CostEstimate(flops=4 * n_tok * width * ff, bytes_accessed=12_000_000, transcendentals=0),
        name='dense_fwd',
    )(x, w_in, w_out)


def tail_kernel(p_own, p_mate, p_far, mid_ref, dy_ref, x_ref, pre_ref, w_in, w_out, dx_ref):
    d_norm = (p_own[...] + p_mate[...] + p_far[...]).astype(bf16)
    d_mid = (dy_ref[...].astype(f32) + rms_back(mid_ref[...].astype(f32), d_norm).astype(f32)).astype(bf16)
    d_hid = dot_nt(d_mid, w_out[...]).astype(bf16).astype(f32)
    pre = pre_ref[...].astype(f32)
    sig = sigmoid(pre)
    d_pre = (d_hid * (sig + pre * sig * (1.0 - sig))).astype(bf16)
    d_in = dot_nt(d_pre, w_in[...]).astype(bf16)
    dx_ref[...] = (d_mid.astype(f32) + rms_back(x_ref[...].astype(f32), d_in).astype(f32)).astype(bf16)


def run_tail(chunk, p_own, p_mate, p_far, mid, dy, x, pre, w_in, w_out):
    n_tok, width = x.shape
    ff = w_in.shape[1]
    steps = 2
    rows = n_tok // TAIL // steps
    row = pl.BlockSpec((rows, width), lambda i: (chunk * steps + i, 0))
    return pl.pallas_call(
        tail_kernel,
        grid=(steps,),
        out_shape=jax.ShapeDtypeStruct((n_tok // TAIL, width), bf16),
        in_specs=[row] * 6 + [pl.BlockSpec((rows, ff), lambda i: (chunk * steps + i, 0)),
                              pl.BlockSpec((width, ff), lambda i: (0, 0)), pl.BlockSpec((ff, width), lambda i: (0, 0))],
        out_specs=pl.BlockSpec((rows, width), lambda i: (i, 0)),
        cost_estimate=pl.CostEstimate(flops=4 * rows * steps * width * ff, bytes_accessed=6_000_000, transcendentals=0),
    )(p_own, p_mate, p_far, mid, dy, x, pre, w_in, w_out)


def run_experts(meta, far, toks, dys, w_own, w_mate, dw_prev):
    starts, nwins, ntiles, base, rank, gate = meta
    bwd = dys is not None
    carry = dw_prev is not None
    half, width = toks[0].shape
    e_loc, _, ff = w_own[0].shape
    smem = pl.BlockSpec(memory_space=pltpu.SMEM)
    vmem = pl.BlockSpec(memory_space=pltpu.VMEM)
    hbm = pl.BlockSpec(memory_space=pl.ANY)
    args = [starts, nwins, ntiles, base, rank, gate, *toks]
    if bwd:
        args += [*dys]
    args += [*w_own, *w_mate]
    if carry:
        args += [*dw_prev]
    in_specs = [smem] * 4 + [vmem] * 2 + [hbm] * (len(args) - 6)
    out_shape = [jax.ShapeDtypeStruct((half, width), f32)] * 2
    if bwd:
        for n in (e_loc, 2):
            out_shape += [jax.ShapeDtypeStruct((n, *w.shape[1:]), f32) for w in w_own]
    rows = SUB * TILE_SUBS[int(bwd)]
    scratch = [
        pltpu.VMEM((2 * half, width), bf16),
        pltpu.VMEM((2 * half, width), f32),
        pltpu.VMEM((2, width, ff), bf16),
        pltpu.VMEM((2, width, ff), bf16),
        pltpu.VMEM((2, ff, width), bf16),
        pltpu.VMEM((rows, width), f32),
        pltpu.VMEM((rows, width), bf16),
    ]
    if bwd:
        scratch += [
            pltpu.VMEM((2 * half, width), bf16),
            pltpu.VMEM((rows, width), f32),
            pltpu.VMEM((width, rows), bf16),
            pltpu.VMEM((rows, ff), bf16),
            pltpu.VMEM((rows, ff), bf16),
            pltpu.VMEM((DW_SLOTS, width, ff), f32),
            pltpu.VMEM((DW_SLOTS, width, ff), f32),
            pltpu.VMEM((DW_SLOTS, ff, width), f32),
            pltpu.SemaphoreType.DMA((2, 2)),
            pltpu.SemaphoreType.DMA((2, 3)),
            pltpu.SemaphoreType.DMA((DW_SLOTS, 3)),
            pltpu.SemaphoreType.DMA((DW_SLOTS, 3)),
        ]
    else:
        scratch += [
            pltpu.VMEM((rows, ff), bf16),
            pltpu.SemaphoreType.DMA((2, 2)),
            pltpu.SemaphoreType.DMA((2, 3)),
        ]
    flops = (8 if bwd else 3) * 2 * 3584 * 2 * width * ff
    return pl.pallas_call(
        functools.partial(expert_kernel, bwd, carry, E_RUN if far else 0),
        out_shape=out_shape,
        in_specs=in_specs,
        out_specs=[hbm] * len(out_shape),
        scratch_shapes=scratch,
        compiler_params=pltpu.CompilerParams(vmem_limit_bytes=60 * 1024 * 1024),
        cost_estimate=pl.CostEstimate(flops=flops, bytes_accessed=60_000_000, transcendentals=0),
        name='experts_bwd' if bwd else 'experts_fwd',
    )(*args)


def solution(mesh):
    n_ep = mesh.shape['ep']
    n_pp = mesh.shape['pp']
    fwd_perm = [(i, (i + 1) % n_pp) for i in range(n_pp)]
    bwd_perm = [(i, (i - 1) % n_pp) for i in range(n_pp)]

    def to_mate(v):
        return lax.ppermute(v, 'ep', [(i, i ^ 1) for i in range(n_ep)])

    def to_cross(v):
        return lax.ppermute(v, 'ep', [(i, i ^ 2) for i in range(n_ep)])

    def device_fn(x_fwd, x_bwd, dy_bwd, ids_fwd, gate_fwd, ids_bwd, gate_bwd, w_in, w_out, w_gate, w_up, w_down):
        fwd_x, bwd_x, bwd_dy = x_fwd[0], x_bwd[0], dy_bwd[0]
        stage_w_in, stage_w_out = w_in[0], w_out[0]
        w_own = (w_gate[0], w_up[0], w_down[0])
        n_tok, _ = fwd_x.shape
        top_k = ids_fwd.shape[2]
        e_loc = w_own[0].shape[0]
        n_exp = e_loc * n_ep
        cap = 3 * n_tok * top_k // n_exp
        me = lax.axis_index('ep')
        core = lax.rem(me, 2)
        base = 2 * core
        n_sub = -(-2 * cap // SUB)

        def gather_pair(v):
            far = to_cross(v)
            return (v, to_mate(v)), (far, to_mate(far))

        fields = [ids_fwd[0].astype(f32).T, gate_fwd[0].astype(f32).T, ids_bwd[0].astype(f32).T, gate_bwd[0].astype(f32).T]
        table = jnp.concatenate(fields)
        tables = [table, to_mate(table), to_cross(table)]
        tables.append(lax.ppermute(table, 'ep', [(i, i ^ 3) for i in range(n_ep)]))
        mine = e_loc * me + base
        mates = e_loc * (me ^ 1) + base
        who = jnp.stack([mine, mine + 1, mates, mates + 1]).astype(i32)
        base_arr = base.reshape(1).astype(i32)
        ranks, gates, starts, nwins, ntiles = run_routing(who, tables, n_sub)
        meta = (starts, nwins, ntiles, base_arr, ranks, gates)

        far_dy = to_cross(bwd_dy)
        dy_near, dy_far = (bwd_dy, to_mate(bwd_dy)), (far_dy, to_mate(far_dy))
        w_mate = tuple(to_mate(w) for w in w_own)

        def combine(parts):
            return parts[0] + to_mate(parts[1])

        norm_f, mid_f = run_dense(fwd_x, stage_w_in, stage_w_out, False)
        near_f, far_f = gather_pair(norm_f)
        norm_b, mid_b, pre_b = run_dense(bwd_x, stage_w_in, stage_w_out, True)
        near_b, far_b = gather_pair(norm_b)

        pf_near = run_experts(meta, False, near_f, None, w_own, w_mate, None)
        pf_far = run_experts(meta, True, far_f, None, w_own, w_mate, None)
        ret_f = to_cross(combine(pf_far))
        pb_far = run_experts(meta, True, far_b, dy_far, w_own, w_mate, None)
        ret_b = to_cross(combine(pb_far[:2]))
        pb_near = run_experts(meta, False, near_b, dy_near, w_own, w_mate, pb_far[2:])
        dw_full, dw_mate = pb_near[2:5], pb_near[5:8]

        near_f_mate = to_mate(pf_near[1])
        y_val = (mid_f.astype(f32) + (pf_near[0] + near_f_mate + ret_f)).astype(bf16)
        y_next = lax.ppermute(y_val, 'pp', fwd_perm)

        dx_parts = []
        from_mate = to_mate(pb_near[1])
        for c in range(TAIL):
            dx_val = run_tail(c, pb_near[0], from_mate, ret_b, mid_b, bwd_dy, bwd_x, pre_b, stage_w_in, stage_w_out)
            dx_parts.append(lax.ppermute(dx_val, 'pp', bwd_perm))
        dx_prev = jnp.concatenate(dx_parts)

        back = [to_mate(v) for v in dw_mate]
        zero = jnp.zeros((), i32)
        dw_gate, dw_up, dw_down = [lax.dynamic_update_slice(full, part, (2 - base, zero, zero)) for full, part in zip(dw_full, back)]
        return y_next[None], dx_prev[None], dw_gate[None], dw_up[None], dw_down[None]

    spec_act = P('pp', 'ep', None)
    spec_dense = P('pp', None, None)
    spec_exp = P('pp', 'ep', None, None)


    return jax.shard_map(device_fn, mesh=mesh, in_specs=(spec_act,) * 7 + (spec_dense,) * 2 + (spec_exp,) * 3, out_specs=(spec_act, spec_act, spec_exp, spec_exp, spec_exp), check_vma=False)
```

```python
import functools

import jax
import jax.numpy as jnp
from jax import lax
from jax.experimental import pallas as pl
from jax.experimental.pallas import tpu as pltpu
from jax.sharding import PartitionSpec as P


EPS_NORM = 1e-6
SUB = 128
TILE_SUBS = (3, 4)
WIN = 256
WIN_MORE = 1536
ALIGN = 64
CHUNK = 256
OUT_ROWS = 512
DW_SLOTS = 3
TAIL = 4
DENSE_ROWS = 512
E_RUN = 4

f32 = jnp.float32
bf16 = jnp.bfloat16
i32 = jnp.int32


def dot_nn(a, b):
    return lax.dot_general(a, b, (((1,), (0,)), ((), ())), preferred_element_type=f32)


def dot_nt(a, b):
    return lax.dot_general(a, b, (((1,), (1,)), ((), ())), preferred_element_type=f32)


def dot_tn(a, b):
    return lax.dot_general(a, b, (((0,), (0,)), ((), ())), preferred_element_type=f32)


def expert_kernel(bwd, carry, row0, *refs):
    refs = list(refs)

    def take(n):
        out = refs[:n]
        del refs[:n]
        return out

    starts, nwins, ntiles, base_ref, rank_ref, gate_ref = take(6)
    tok_in = take(2)
    dy_in = take(2) if bwd else []
    mb = int(bwd)
    per_tile = TILE_SUBS[mb]
    w_own = take(3)
    w_mate = take(3)
    dw_in = take(6) if carry else []
    p_out = take(2)
    dw_out = take(6) if bwd else []
    order, tok, acc, wg_buf, wu_buf, wd_buf, x_acc, out_all = take(8)
    if bwd:
        dyt, d_acc, xt, dg_all, du_all, dwg_buf, dwu_buf, dwd_buf = take(8)
        tok_sem, w_sem, in_sem, out_sem = take(4)
    else:
        (act_all,) = take(1)
        tok_sem, w_sem = take(2)
    half = tok_in[0].shape[0]
    n_tok = 2 * half
    ff = wg_buf.shape[2]
    base = base_ref[0]

    loads = []
    for i, (src, dst) in enumerate([(tok_in, tok)] + ([(dy_in, dyt)] if bwd else [])):
        for j in range(2):
            loads.append(pltpu.make_async_copy(src[j], dst.at[pl.ds(j * half, half), :], tok_sem.at[i, j]))
    for c in loads:
        c.start()

    def w_copies(srcs, idx, slot):
        return [pltpu.make_async_copy(s.at[idx], b.at[slot], w_sem.at[slot, k])
                for k, (s, b) in enumerate(zip(srcs, (wg_buf, wu_buf, wd_buf)))]

    def w_start(e, slot):
        @pl.when(e < 2)
        def _():
            for c in w_copies(w_own, base + e, slot):
                c.start()

        @pl.when(e >= 2)
        def _():
            for c in w_copies(w_mate, base + e - 2, slot):
                c.start()

    def dw_copies(refs6, e, slot, sem, inward):
        bufs = (dwg_buf, dwu_buf, dwd_buf)

        def go(refs3, idx, what):
            for k in range(3):
                hbm, buf = refs3[k].at[idx], bufs[k].at[slot]
                c = pltpu.make_async_copy(hbm, buf, sem.at[slot, k]) if inward else pltpu.make_async_copy(buf, hbm, sem.at[slot, k])
                getattr(c, what)()

        def start():
            @pl.when(e < 2)
            def _():
                go(refs6[:3], base + e, 'start')

            @pl.when(e >= 2)
            def _():
                go(refs6[3:], e - 2, 'start')

        def wait():
            go(refs6[3:], 0, 'wait')

        return start, wait

    tiles_of = [ntiles[mb, row0 + e, 0] for e in range(E_RUN)]
    for e in range(E_RUN):
        rank = 0
        for o in range(E_RUN):
            if o != e:
                ahead = tiles_of[o] >= tiles_of[e] if o < e else tiles_of[o] > tiles_of[e]
                rank = rank + ahead.astype(i32)
        place = jnp.where(rank == 0, 0, jnp.where(rank == 1, E_RUN - 1, rank - 1))
        order[place] = e

    def clear(ref):
        rows = 64

        @pl.loop(0, ref.shape[0] // rows)
        def _(k):
            ref[pl.ds(pl.multiple_of(k * rows, rows), rows), :] = jnp.zeros((rows, ref.shape[1]), ref.dtype)

    w_start(order[0], 0)
    if carry:
        dw_copies(dw_in, order[0], 0, in_sem, True)[0]()
    clear(acc)
    for c in loads:
        c.wait()

    def window(e, st, k):
        size = WIN_MORE if k is not None else WIN
        so = starts[mb, row0 + e, st]
        if k is not None:
            so += WIN + (k - 1) * WIN_MORE
        s = jnp.minimum(so, n_tok - size)
        shift = lax.rem(s // ALIGN, 2)
        lanes = pl.ds(pl.multiple_of(s - shift * ALIGN, 128), size)
        rk = rank_ref[mb, shift, pl.ds(row0 + e, 1), lanes]
        lane = lax.broadcasted_iota(i32, (1, size), 1) + s
        rk = jnp.where(lane >= so, rk, -1) - st * SUB
        mask = lax.broadcasted_iota(i32, (SUB, size), 0) == rk
        toks = pl.ds(pl.multiple_of(s, ALIGN), size)
        return toks, lambda: jnp.where(mask, 1.0, 0.0).astype(bf16), \
            lambda: jnp.where(mask, gate_ref[mb, shift, pl.ds(row0 + e, 1), lanes], 0.0).astype(bf16)

    def p_copy(q):
        per = half // OUT_ROWS
        for j in range(2):
            @pl.when(q // per == j)
            def _():
                dst = p_out[j].at[pl.ds(pl.multiple_of((q - j * per) * OUT_ROWS, OUT_ROWS), OUT_ROWS), :]
                pltpu.make_async_copy(acc.at[pl.ds(pl.multiple_of(q * OUT_ROWS, OUT_ROWS), OUT_ROWS), :], dst, tok_sem.at[0, j]).start()

    def expert(i, _):
        e = order[i]
        slot = lax.rem(i, 2)
        for c in w_copies(w_own, 0, slot):
            c.wait()

        @pl.when(i < E_RUN - 1)
        def _():
            w_start(order[i + 1], 1 - slot)

        wg, wu, wd = wg_buf.at[slot], wu_buf.at[slot], wd_buf.at[slot]
        if bwd:
            d_slot = lax.rem(i, DW_SLOTS)

            @pl.when(i >= 2)
            def _():
                dw_copies(dw_out, 0, lax.rem(i - 2, DW_SLOTS), out_sem, False)[1]()

            if carry:
                @pl.when(i < E_RUN - 1)
                def _():
                    dw_copies(dw_in, order[i + 1], lax.rem(i + 1, DW_SLOTS), in_sem, True)[0]()

                dw_copies(dw_in, e, d_slot, in_sem, True)[1]()
            else:
                for b in (dwg_buf, dwu_buf, dwd_buf):
                    clear(b.at[d_slot])
            dwg, dwu, dwd = dwg_buf.at[d_slot], dwu_buf.at[d_slot], dwd_buf.at[d_slot]

        def tile(t, _):
            for h in range(per_tile):
                rows = pl.ds(h * SUB, SUB)
                toks, ones, gated = window(e, t * per_tile + h, None)
                x_acc[rows, :] = dot_nn(ones(), tok[toks, :])
                if bwd:
                    d_acc[rows, :] = dot_nn(gated(), dyt[toks, :])

            n_win = nwins[mb, row0 + e, t * per_tile]
            for h in range(1, per_tile):
                n_win = jnp.maximum(n_win, nwins[mb, row0 + e, t * per_tile + h])

            @pl.when(n_win > 1)
            def _():
                @pl.loop(0, per_tile)
                def _(h):
                    st = t * per_tile + h
                    rows = pl.ds(pl.multiple_of(h * SUB, SUB), SUB)

                    @pl.loop(1, nwins[mb, row0 + e, st])
                    def _(k):
                        toks, ones, gated = window(e, st, k)
                        x_acc[rows, :] += dot_nn(ones(), tok[toks, :])
                        if bwd:
                            d_acc[rows, :] += dot_nn(gated(), dyt[toks, :])

            x = x_acc[...].astype(bf16)
            if bwd:
                d = d_acc[...].astype(bf16)
                xt[...] = x.T
            for c in range(0, ff, CHUNK):
                cols = pl.ds(c, CHUNK)
                gp = dot_nn(x, wg[:, cols]).astype(bf16).astype(f32)
                up = dot_nn(x, wu[:, cols]).astype(bf16).astype(f32)
                sig = 1.0 / (1.0 + jnp.exp(-gp))
                silu = gp * sig
                if not bwd:
                    act_all[:, cols] = (silu * up).astype(bf16)
                    continue
                da = dot_nt(d, wd[cols, :]).astype(bf16).astype(f32)
                act = (silu * up).astype(bf16)
                du = (da * silu).astype(bf16)
                dg = (da * up * (sig + silu * (1.0 - sig))).astype(bf16)
                dg_all[:, cols] = dg
                du_all[:, cols] = du
                dwd[cols, :] += dot_tn(act, d)
                dwg[:, cols] += dot_nn(xt[...], dg)
                dwu[:, cols] += dot_nn(xt[...], du)
            if bwd:
                out = (dot_nt(dg_all[...], wg[...]) + dot_nt(du_all[...], wu[...])).astype(bf16)
            else:
                out = dot_nn(act_all[...], wd[...]).astype(bf16)

            def put(st, k, part):
                toks, ones, gated = window(e, st, k)
                acc[toks, :] += dot_tn(ones() if bwd else gated(), part)

            out_all[...] = out
            for h in range(per_tile):
                put(t * per_tile + h, None, out[h * SUB:(h + 1) * SUB, :])

            @pl.when(n_win > 1)
            def _():
                @pl.loop(0, per_tile)
                def _(h):
                    st = t * per_tile + h

                    @pl.loop(1, nwins[mb, row0 + e, st])
                    def _(k):
                        put(st, k, out_all[pl.ds(pl.multiple_of(h * SUB, SUB), SUB), :])

            @pl.when(i == E_RUN - 1)
            def _():
                def final(tile_idx):
                    return jnp.minimum(starts[mb, row0 + e, tile_idx * per_tile], n_tok - WIN_MORE) // OUT_ROWS

                lo = jnp.where(t == 0, 0, final(t))
                hi = jnp.where(t == ntiles[mb, row0 + e, 0] - 1, n_tok // OUT_ROWS, final(t + 1))

                @pl.loop(lo, hi)
                def _(q):
                    p_copy(q)

            return 0

        lax.fori_loop(0, ntiles[mb, row0 + e, 0], tile, 0)
        if bwd:
            dw_copies(dw_out, e, d_slot, out_sem, False)[0]()
        return 0

    lax.fori_loop(0, E_RUN, expert, 0)
    outs = [pltpu.make_async_copy(acc.at[pl.ds(j * half, half), :], p_out[j], tok_sem.at[0, j]) for j in range(2)]
    if bwd:
        for e in (E_RUN - 2, E_RUN - 1):
            dw_copies(dw_out, e, e % DW_SLOTS, out_sem, False)[1]()
    for c in outs:
        c.wait()


def routing_kernel(n_sub, who_ref, tab0, tab1, tab2, tab3, rank_ref, gate_ref, start_ref, nwin_ref, ntile_ref, hit_ref):
    fields, n_tok = tab0.shape
    top_k = fields // 4
    n2 = 2 * n_tok
    n_blk = n2 // 128
    r_i = lax.broadcasted_iota(i32, (128, 128), 0)
    c_i = lax.broadcasted_iota(i32, (128, 128), 1)
    tri = jnp.where(r_i <= c_i, 1.0, 0.0).astype(bf16)
    full = jnp.ones((128, 128), bf16)
    lane = lax.broadcasted_iota(i32, (2 * E_RUN, 128), 1)
    for mb in range(2):
        for q, tab in enumerate((tab0, tab1, tab2, tab3)):
            part = tab[mb * 2 * top_k:(mb + 1) * 2 * top_k, :]
            ids, gates = part[:top_k], part[top_k:]
            cols = pl.ds((q % 2) * n_tok, n_tok)
            for e in range(E_RUN):
                match = ids == who_ref[e].astype(f32)
                row = (q // 2) * E_RUN + e
                hit_ref[row:row + 1, cols] = jnp.sum(jnp.where(match, 1.0, 0.0), axis=0, keepdims=True)
                gate_ref[mb, 0, row:row + 1, cols] = jnp.sum(jnp.where(match, gates, 0.0), axis=0, keepdims=True)
        hits = [hit_ref[:, b * 128:(b + 1) * 128] for b in range(n_blk)]
        stacked = jnp.concatenate(hits, axis=0).astype(bf16)
        within = dot_nn(stacked, tri)
        totals = dot_nn(stacked, full)
        carry = jnp.zeros((2 * E_RUN, 128), f32)
        incl = []
        for b in range(n_blk):
            rows = slice(b * 2 * E_RUN, (b + 1) * 2 * E_RUN)
            v = (within[rows] + carry).astype(i32)
            rank_ref[mb, 0, :, b * 128:(b + 1) * 128] = jnp.where(hits[b] > 0.5, v - 1, -1)
            incl.append(v)
            carry = carry + totals[rows]
        for ref, fill in ((rank_ref, -1), (gate_ref, 0.0)):
            ref[mb, 1, :, :n2 - 128] = ref[mb, 0, :, ALIGN:n2 - 128 + ALIGN]
            tail = jnp.concatenate([ref[mb, 0, :, n2 - 128:], jnp.full((2 * E_RUN, 128), fill, ref.dtype)], axis=1)
            ref[mb, 1, :, n2 - 128:] = tail[:, ALIGN:128 + ALIGN]
        cnt = carry.astype(i32)

        def tokens_upto(limit):
            tot = jnp.zeros((2 * E_RUN, 128), f32)
            for v in incl:
                tot = tot + jnp.where(v <= limit, 1.0, 0.0)
            return jnp.sum(tot, axis=1, keepdims=True).astype(i32)

        start = jnp.zeros((2 * E_RUN, 128), i32)
        nwin = jnp.ones((2 * E_RUN, 128), i32)
        for j in range(n_sub):
            lo = jnp.minimum(tokens_upto(j * SUB), n2 - 1) // ALIGN * ALIGN
            hi = tokens_upto(jnp.minimum((j + 1) * SUB, cnt) - 1) + 1
            n = jnp.maximum((hi - lo - WIN + WIN_MORE - 1) // WIN_MORE, 0) + 1
            start = jnp.where(lane == j, lo, start)
            nwin = jnp.where(lane == j, n, nwin)
        start_ref[mb] = start
        nwin_ref[mb] = nwin
        tile_rows = SUB * TILE_SUBS[mb]
        ntile_ref[mb] = jnp.maximum((cnt + tile_rows - 1) // tile_rows, 1)


def run_routing(who, tables, n_sub):
    n_tok = tables[0].shape[1]
    rows = 2 * E_RUN
    wide = (2, 2, rows, 2 * n_tok)
    small = jax.ShapeDtypeStruct((2, rows, 128), i32)
    vmem = pl.BlockSpec(memory_space=pltpu.VMEM)
    return pl.pallas_call(
        functools.partial(routing_kernel, n_sub),
        out_shape=[jax.ShapeDtypeStruct(wide, i32), jax.ShapeDtypeStruct(wide, f32), small, small, small],
        in_specs=[pl.BlockSpec(memory_space=pltpu.SMEM)] + [vmem] * 4,
        out_specs=[vmem] * 5,
        scratch_shapes=[pltpu.VMEM((rows, 2 * n_tok), f32)],
        name='routing',
    )(who, *tables)


def sigmoid(v):
    return 1.0 / (1.0 + jnp.exp(-v))


def rms_scale(rows_f32):
    return lax.rsqrt(jnp.mean(rows_f32 * rows_f32, axis=-1, keepdims=True) + EPS_NORM)


def rms_back(rows_f32, cot):
    cot = cot.astype(f32)
    scale = rms_scale(rows_f32)
    proj = jnp.mean(cot * rows_f32, axis=-1, keepdims=True)
    return (scale * cot - rows_f32 * (scale * scale * scale * proj)).astype(bf16)


def dense_kernel(x_ref, w_in, w_out, norm_ref, mid_ref, *rest):
    *pre_ref, hid = rest
    x = x_ref[...].astype(f32)
    norm_in = (x * rms_scale(x)).astype(bf16)
    for c in range(0, w_in.shape[1], CHUNK):
        cols = pl.ds(c, CHUNK)
        pre = dot_nn(norm_in, w_in[:, cols]).astype(bf16)
        if pre_ref:
            pre_ref[0][:, cols] = pre
        pre = pre.astype(f32)
        hid[:, cols] = (pre * sigmoid(pre)).astype(bf16)
    mid = (x_ref[...].astype(f32) + dot_nn(hid[...], w_out[...])).astype(bf16)
    mid_ref[...] = mid
    mid = mid.astype(f32)
    norm_ref[...] = (mid * rms_scale(mid)).astype(bf16)


def run_dense(x, w_in, w_out, keep_pre):
    n_tok, width = x.shape
    ff = w_in.shape[1]
    row = pl.BlockSpec((DENSE_ROWS, width), lambda i: (i, 0))
    out_shape = [jax.ShapeDtypeStruct(x.shape, bf16)] * 2
    out_specs = [row, row]
    if keep_pre:
        out_shape += [jax.ShapeDtypeStruct((n_tok, ff), bf16)]
        out_specs += [pl.BlockSpec((DENSE_ROWS, ff), lambda i: (i, 0))]
    return pl.pallas_call(
        dense_kernel,
        grid=(n_tok // DENSE_ROWS,),
        out_shape=out_shape,
        in_specs=[row, pl.BlockSpec((width, ff), lambda i: (0, 0)), pl.BlockSpec((ff, width), lambda i: (0, 0))],
        out_specs=out_specs,
        scratch_shapes=[pltpu.VMEM((DENSE_ROWS, ff), bf16)],
        cost_estimate=pl.CostEstimate(flops=4 * n_tok * width * ff, bytes_accessed=12_000_000, transcendentals=0),
        name='dense_fwd',
    )(x, w_in, w_out)


def tail_kernel(p_own, p_mate, p_far, mid_ref, dy_ref, x_ref, pre_ref, w_in, w_out, dx_ref, d_all):
    d_norm = (p_own[...] + p_mate[...] + p_far[...]).astype(bf16)
    d_mid = (dy_ref[...].astype(f32) + rms_back(mid_ref[...].astype(f32), d_norm).astype(f32)).astype(bf16)
    for c in range(0, w_in.shape[1], CHUNK):
        cols = pl.ds(c, CHUNK)
        d_hid = dot_nt(d_mid, w_out[cols, :]).astype(bf16).astype(f32)
        pre = pre_ref[:, cols].astype(f32)
        sig = sigmoid(pre)
        d_all[:, cols] = (d_hid * (sig + pre * sig * (1.0 - sig))).astype(bf16)
    d_in = dot_nt(d_all[...], w_in[...]).astype(bf16)
    dx_ref[...] = (d_mid.astype(f32) + rms_back(x_ref[...].astype(f32), d_in).astype(f32)).astype(bf16)


def run_tail(chunk, p_own, p_mate, p_far, mid, dy, x, pre, w_in, w_out):
    n_tok, width = x.shape
    ff = w_in.shape[1]
    steps = 2
    rows = n_tok // TAIL // steps
    row = pl.BlockSpec((rows, width), lambda i: (chunk * steps + i, 0))
    return pl.pallas_call(
        tail_kernel,
        grid=(steps,),
        out_shape=jax.ShapeDtypeStruct((n_tok // TAIL, width), bf16),
        in_specs=[row] * 6 + [pl.BlockSpec((rows, ff), lambda i: (chunk * steps + i, 0)),
                              pl.BlockSpec((width, ff), lambda i: (0, 0)), pl.BlockSpec((ff, width), lambda i: (0, 0))],
        out_specs=pl.BlockSpec((rows, width), lambda i: (i, 0)),
        scratch_shapes=[pltpu.VMEM((rows, ff), bf16)],
        cost_estimate=pl.CostEstimate(flops=4 * rows * steps * width * ff, bytes_accessed=6_000_000, transcendentals=0),
    )(p_own, p_mate, p_far, mid, dy, x, pre, w_in, w_out)


def run_experts(meta, far, toks, dys, w_own, w_mate, dw_prev):
    starts, nwins, ntiles, base, rank, gate = meta
    bwd = dys is not None
    carry = dw_prev is not None
    half, width = toks[0].shape
    e_loc, _, ff = w_own[0].shape
    smem = pl.BlockSpec(memory_space=pltpu.SMEM)
    vmem = pl.BlockSpec(memory_space=pltpu.VMEM)
    hbm = pl.BlockSpec(memory_space=pl.ANY)
    args = [starts, nwins, ntiles, base, rank, gate, *toks]
    if bwd:
        args += [*dys]
    args += [*w_own, *w_mate]
    if carry:
        args += [*dw_prev]
    in_specs = [smem] * 4 + [vmem] * 2 + [hbm] * (len(args) - 6)
    out_shape = [jax.ShapeDtypeStruct((half, width), f32)] * 2
    if bwd:
        for n in (e_loc, 2):
            out_shape += [jax.ShapeDtypeStruct((n, *w.shape[1:]), f32) for w in w_own]
    rows = SUB * TILE_SUBS[int(bwd)]
    scratch = [
        pltpu.SMEM((E_RUN,), i32),
        pltpu.VMEM((2 * half, width), bf16),
        pltpu.VMEM((2 * half, width), f32),
        pltpu.VMEM((2, width, ff), bf16),
        pltpu.VMEM((2, width, ff), bf16),
        pltpu.VMEM((2, ff, width), bf16),
        pltpu.VMEM((rows, width), f32),
        pltpu.VMEM((rows, width), bf16),
    ]
    if bwd:
        scratch += [
            pltpu.VMEM((2 * half, width), bf16),
            pltpu.VMEM((rows, width), f32),
            pltpu.VMEM((width, rows), bf16),
            pltpu.VMEM((rows, ff), bf16),
            pltpu.VMEM((rows, ff), bf16),
            pltpu.VMEM((DW_SLOTS, width, ff), f32),
            pltpu.VMEM((DW_SLOTS, width, ff), f32),
            pltpu.VMEM((DW_SLOTS, ff, width), f32),
            pltpu.SemaphoreType.DMA((2, 2)),
            pltpu.SemaphoreType.DMA((2, 3)),
            pltpu.SemaphoreType.DMA((DW_SLOTS, 3)),
            pltpu.SemaphoreType.DMA((DW_SLOTS, 3)),
        ]
    else:
        scratch += [
            pltpu.VMEM((rows, ff), bf16),
            pltpu.SemaphoreType.DMA((2, 2)),
            pltpu.SemaphoreType.DMA((2, 3)),
        ]
    flops = (8 if bwd else 3) * 2 * 3584 * 2 * width * ff
    return pl.pallas_call(
        functools.partial(expert_kernel, bwd, carry, E_RUN if far else 0),
        out_shape=out_shape,
        in_specs=in_specs,
        out_specs=[hbm] * len(out_shape),
        scratch_shapes=scratch,
        compiler_params=pltpu.CompilerParams(vmem_limit_bytes=60 * 1024 * 1024),
        cost_estimate=pl.CostEstimate(flops=flops, bytes_accessed=60_000_000, transcendentals=0),
        name='experts_bwd' if bwd else 'experts_fwd',
    )(*args)


def solution(mesh):
    n_ep = mesh.shape['ep']
    n_pp = mesh.shape['pp']
    fwd_perm = [(i, (i + 1) % n_pp) for i in range(n_pp)]
    bwd_perm = [(i, (i - 1) % n_pp) for i in range(n_pp)]

    def to_mate(v):
        return lax.ppermute(v, 'ep', [(i, i ^ 1) for i in range(n_ep)])

    def to_cross(v):
        return lax.ppermute(v, 'ep', [(i, i ^ 2) for i in range(n_ep)])

    def device_fn(x_fwd, x_bwd, dy_bwd, ids_fwd, gate_fwd, ids_bwd, gate_bwd, w_in, w_out, w_gate, w_up, w_down):
        fwd_x, bwd_x, bwd_dy = x_fwd[0], x_bwd[0], dy_bwd[0]
        stage_w_in, stage_w_out = w_in[0], w_out[0]
        w_own = (w_gate[0], w_up[0], w_down[0])
        n_tok, _ = fwd_x.shape
        top_k = ids_fwd.shape[2]
        e_loc = w_own[0].shape[0]
        n_exp = e_loc * n_ep
        cap = 3 * n_tok * top_k // n_exp
        me = lax.axis_index('ep')
        core = lax.rem(me, 2)
        base = 2 * core
        n_sub = -(-2 * cap // SUB)

        def gather_pair(v):
            far = to_cross(v)
            return (v, to_mate(v)), (far, to_mate(far))

        fields = [ids_fwd[0].astype(f32).T, gate_fwd[0].astype(f32).T, ids_bwd[0].astype(f32).T, gate_bwd[0].astype(f32).T]
        table = jnp.concatenate(fields)
        tables = [table, to_mate(table), to_cross(table)]
        tables.append(lax.ppermute(table, 'ep', [(i, i ^ 3) for i in range(n_ep)]))
        mine = e_loc * me + base
        mates = e_loc * (me ^ 1) + base
        who = jnp.stack([mine, mine + 1, mates, mates + 1]).astype(i32)
        base_arr = base.reshape(1).astype(i32)
        ranks, gates, starts, nwins, ntiles = run_routing(who, tables, n_sub)
        meta = (starts, nwins, ntiles, base_arr, ranks, gates)

        far_dy = to_cross(bwd_dy)
        dy_near, dy_far = (bwd_dy, to_mate(bwd_dy)), (far_dy, to_mate(far_dy))
        w_mate = tuple(to_mate(w) for w in w_own)

        def combine(parts):
            return parts[0] + to_mate(parts[1])

        norm_f, mid_f = run_dense(fwd_x, stage_w_in, stage_w_out, False)
        near_f, far_f = gather_pair(norm_f)
        norm_b, mid_b, pre_b = run_dense(bwd_x, stage_w_in, stage_w_out, True)
        near_b, far_b = gather_pair(norm_b)

        pf_near = run_experts(meta, False, near_f, None, w_own, w_mate, None)
        pf_far = run_experts(meta, True, far_f, None, w_own, w_mate, None)
        ret_f = to_cross(combine(pf_far))
        pb_far = run_experts(meta, True, far_b, dy_far, w_own, w_mate, None)
        ret_b = to_cross(combine(pb_far[:2]))
        pb_near = run_experts(meta, False, near_b, dy_near, w_own, w_mate, pb_far[2:])
        dw_full, dw_mate = pb_near[2:5], pb_near[5:8]

        near_f_mate = to_mate(pf_near[1])
        y_val = (mid_f.astype(f32) + (pf_near[0] + near_f_mate + ret_f)).astype(bf16)
        y_next = lax.ppermute(y_val, 'pp', fwd_perm)

        dx_parts = []
        from_mate = to_mate(pb_near[1])
        for c in range(TAIL):
            dx_val = run_tail(c, pb_near[0], from_mate, ret_b, mid_b, bwd_dy, bwd_x, pre_b, stage_w_in, stage_w_out)
            dx_parts.append(lax.ppermute(dx_val, 'pp', bwd_perm))
        dx_prev = jnp.concatenate(dx_parts)

        back = [to_mate(v) for v in dw_mate]
        zero = jnp.zeros((), i32)
        dw_gate, dw_up, dw_down = [lax.dynamic_update_slice(full, part, (2 - base, zero, zero)) for full, part in zip(dw_full, back)]
        return y_next[None], dx_prev[None], dw_gate[None], dw_up[None], dw_down[None]

    spec_act = P('pp', 'ep', None)
    spec_dense = P('pp', None, None)
    spec_exp = P('pp', 'ep', None, None)


    return jax.shard_map(device_fn, mesh=mesh, in_specs=(spec_act,) * 7 + (spec_dense,) * 2 + (spec_exp,) * 3, out_specs=(spec_act, spec_act, spec_exp, spec_exp, spec_exp), check_vma=False)
```

```python
import functools

import jax
import jax.numpy as jnp
from jax import lax
from jax.experimental import pallas as pl
from jax.experimental.pallas import tpu as pltpu
from jax.sharding import PartitionSpec as P


EPS_NORM = 1e-6
SUB = 128
TILE_SUBS = (3, 4)
WIN = 256
WIN_MORE = 1536
ALIGN = 64
CHUNK = 256
OUT_ROWS = 512
DW_SLOTS = 3
TAIL = (0, 1, 3, 5, 8)
DENSE_ROWS = 512
E_RUN = 4

f32 = jnp.float32
bf16 = jnp.bfloat16
i32 = jnp.int32


def dot_nn(a, b):
    return lax.dot_general(a, b, (((1,), (0,)), ((), ())), preferred_element_type=f32)


def dot_nt(a, b):
    return lax.dot_general(a, b, (((1,), (1,)), ((), ())), preferred_element_type=f32)


def dot_tn(a, b):
    return lax.dot_general(a, b, (((0,), (0,)), ((), ())), preferred_element_type=f32)


def expert_kernel(bwd, carry, row0, *refs):
    refs = list(refs)

    def take(n):
        out = refs[:n]
        del refs[:n]
        return out

    starts, nwins, ntiles, base_ref, rank_ref, gate_ref = take(6)
    tok_in = take(2)
    dy_in = take(2) if bwd else []
    mb = int(bwd)
    per_tile = TILE_SUBS[mb]
    w_own = take(3)
    w_mate = take(3)
    dw_in = take(6) if carry else []
    p_out = take(2)
    dw_out = take(6) if bwd else []
    order, tok, acc, wg_buf, wu_buf, wd_buf, x_acc, out_all = take(8)
    if bwd:
        dyt, d_acc, xt, dg_all, du_all, dwg_buf, dwu_buf, dwd_buf = take(8)
        tok_sem, w_sem, in_sem, out_sem = take(4)
    else:
        (act_all,) = take(1)
        tok_sem, w_sem = take(2)
    half = tok_in[0].shape[0]
    n_tok = 2 * half
    ff = wg_buf.shape[2]
    base = base_ref[0]

    loads = []
    for i, (src, dst) in enumerate([(tok_in, tok)] + ([(dy_in, dyt)] if bwd else [])):
        for j in range(2):
            loads.append(pltpu.make_async_copy(src[j], dst.at[pl.ds(j * half, half), :], tok_sem.at[i, j]))
    for c in loads:
        c.start()

    def w_copies(srcs, idx, slot):
        return [pltpu.make_async_copy(s.at[idx], b.at[slot], w_sem.at[slot, k])
                for k, (s, b) in enumerate(zip(srcs, (wg_buf, wu_buf, wd_buf)))]

    def w_start(e, slot):
        @pl.when(e < 2)
        def _():
            for c in w_copies(w_own, base + e, slot):
                c.start()

        @pl.when(e >= 2)
        def _():
            for c in w_copies(w_mate, base + e - 2, slot):
                c.start()

    def dw_copies(refs6, e, slot, sem, inward):
        bufs = (dwg_buf, dwu_buf, dwd_buf)

        def go(refs3, idx, what):
            for k in range(3):
                hbm, buf = refs3[k].at[idx], bufs[k].at[slot]
                c = pltpu.make_async_copy(hbm, buf, sem.at[slot, k]) if inward else pltpu.make_async_copy(buf, hbm, sem.at[slot, k])
                getattr(c, what)()

        def start():
            @pl.when(e < 2)
            def _():
                go(refs6[:3], base + e, 'start')

            @pl.when(e >= 2)
            def _():
                go(refs6[3:], e - 2, 'start')

        def wait():
            go(refs6[3:], 0, 'wait')

        return start, wait

    tiles_of = [ntiles[mb, row0 + e, 0] for e in range(E_RUN)]
    for e in range(E_RUN):
        rank = 0
        for o in range(E_RUN):
            if o != e:
                ahead = tiles_of[o] >= tiles_of[e] if o < e else tiles_of[o] > tiles_of[e]
                rank = rank + ahead.astype(i32)
        place = jnp.where(rank == 0, 0, jnp.where(rank == 1, E_RUN - 1, rank - 1))
        order[place] = e

    def clear(ref):
        rows = 64

        @pl.loop(0, ref.shape[0] // rows)
        def _(k):
            ref[pl.ds(pl.multiple_of(k * rows, rows), rows), :] = jnp.zeros((rows, ref.shape[1]), ref.dtype)

    w_start(order[0], 0)
    if carry:
        dw_copies(dw_in, order[0], 0, in_sem, True)[0]()
    clear(acc)
    for c in loads:
        c.wait()

    def window(e, st, k):
        size = WIN_MORE if k is not None else WIN
        so = starts[mb, row0 + e, st]
        if k is not None:
            so += WIN + (k - 1) * WIN_MORE
        s = jnp.minimum(so, n_tok - size)
        shift = lax.rem(s // ALIGN, 2)
        lanes = pl.ds(pl.multiple_of(s - shift * ALIGN, 128), size)
        rk = rank_ref[mb, shift, pl.ds(row0 + e, 1), lanes]
        lane = lax.broadcasted_iota(i32, (1, size), 1) + s
        rk = jnp.where(lane >= so, rk, -1) - st * SUB
        mask = lax.broadcasted_iota(i32, (SUB, size), 0) == rk
        toks = pl.ds(pl.multiple_of(s, ALIGN), size)
        return toks, lambda: jnp.where(mask, 1.0, 0.0).astype(bf16), \
            lambda: jnp.where(mask, gate_ref[mb, shift, pl.ds(row0 + e, 1), lanes], 0.0).astype(bf16)

    def p_copy(q):
        per = half // OUT_ROWS
        for j in range(2):
            @pl.when(q // per == j)
            def _():
                dst = p_out[j].at[pl.ds(pl.multiple_of((q - j * per) * OUT_ROWS, OUT_ROWS), OUT_ROWS), :]
                pltpu.make_async_copy(acc.at[pl.ds(pl.multiple_of(q * OUT_ROWS, OUT_ROWS), OUT_ROWS), :], dst, tok_sem.at[0, j]).start()

    def expert(i, _):
        e = order[i]
        slot = lax.rem(i, 2)
        for c in w_copies(w_own, 0, slot):
            c.wait()

        @pl.when(i < E_RUN - 1)
        def _():
            w_start(order[i + 1], 1 - slot)

        wg, wu, wd = wg_buf.at[slot], wu_buf.at[slot], wd_buf.at[slot]
        if bwd:
            d_slot = lax.rem(i, DW_SLOTS)

            @pl.when(i >= 2)
            def _():
                dw_copies(dw_out, 0, lax.rem(i - 2, DW_SLOTS), out_sem, False)[1]()

            if carry:
                @pl.when(i < E_RUN - 1)
                def _():
                    dw_copies(dw_in, order[i + 1], lax.rem(i + 1, DW_SLOTS), in_sem, True)[0]()

                dw_copies(dw_in, e, d_slot, in_sem, True)[1]()
            else:
                for b in (dwg_buf, dwu_buf, dwd_buf):
                    clear(b.at[d_slot])
            dwg, dwu, dwd = dwg_buf.at[d_slot], dwu_buf.at[d_slot], dwd_buf.at[d_slot]

        def tile(t, _):
            for h in range(per_tile):
                rows = pl.ds(h * SUB, SUB)
                toks, ones, gated = window(e, t * per_tile + h, None)
                x_acc[rows, :] = dot_nn(ones(), tok[toks, :])
                if bwd:
                    d_acc[rows, :] = dot_nn(gated(), dyt[toks, :])

            n_win = nwins[mb, row0 + e, t * per_tile]
            for h in range(1, per_tile):
                n_win = jnp.maximum(n_win, nwins[mb, row0 + e, t * per_tile + h])

            @pl.when(n_win > 1)
            def _():
                @pl.loop(0, per_tile)
                def _(h):
                    st = t * per_tile + h
                    rows = pl.ds(pl.multiple_of(h * SUB, SUB), SUB)

                    @pl.loop(1, nwins[mb, row0 + e, st])
                    def _(k):
                        toks, ones, gated = window(e, st, k)
                        x_acc[rows, :] += dot_nn(ones(), tok[toks, :])
                        if bwd:
                            d_acc[rows, :] += dot_nn(gated(), dyt[toks, :])

            x = x_acc[...].astype(bf16)
            if bwd:
                d = d_acc[...].astype(bf16)
                xt[...] = x.T
            for c in range(0, ff, CHUNK):
                cols = pl.ds(c, CHUNK)
                gp = dot_nn(x, wg[:, cols]).astype(bf16).astype(f32)
                up = dot_nn(x, wu[:, cols]).astype(bf16).astype(f32)
                sig = 1.0 / (1.0 + jnp.exp(-gp))
                silu = gp * sig
                if not bwd:
                    act_all[:, cols] = (silu * up).astype(bf16)
                    continue
                da = dot_nt(d, wd[cols, :]).astype(bf16).astype(f32)
                act = (silu * up).astype(bf16)
                du = (da * silu).astype(bf16)
                dg = (da * up * (sig + silu * (1.0 - sig))).astype(bf16)
                dg_all[:, cols] = dg
                du_all[:, cols] = du
                dwd[cols, :] += dot_tn(act, d)
                dwg[:, cols] += dot_nn(xt[...], dg)
                dwu[:, cols] += dot_nn(xt[...], du)
            if bwd:
                out = (dot_nt(dg_all[...], wg[...]) + dot_nt(du_all[...], wu[...])).astype(bf16)
            else:
                out = dot_nn(act_all[...], wd[...]).astype(bf16)

            def put(st, k, part):
                toks, ones, gated = window(e, st, k)
                acc[toks, :] += dot_tn(ones() if bwd else gated(), part)

            out_all[...] = out
            for h in range(per_tile):
                put(t * per_tile + h, None, out[h * SUB:(h + 1) * SUB, :])

            @pl.when(n_win > 1)
            def _():
                @pl.loop(0, per_tile)
                def _(h):
                    st = t * per_tile + h

                    @pl.loop(1, nwins[mb, row0 + e, st])
                    def _(k):
                        put(st, k, out_all[pl.ds(pl.multiple_of(h * SUB, SUB), SUB), :])

            @pl.when(i == E_RUN - 1)
            def _():
                def final(tile_idx):
                    return jnp.minimum(starts[mb, row0 + e, tile_idx * per_tile], n_tok - WIN_MORE) // OUT_ROWS

                lo = jnp.where(t == 0, 0, final(t))
                hi = jnp.where(t == ntiles[mb, row0 + e, 0] - 1, n_tok // OUT_ROWS, final(t + 1))

                @pl.loop(lo, hi)
                def _(q):
                    p_copy(q)

            return 0

        lax.fori_loop(0, ntiles[mb, row0 + e, 0], tile, 0)
        if bwd:
            dw_copies(dw_out, e, d_slot, out_sem, False)[0]()
        return 0

    lax.fori_loop(0, E_RUN, expert, 0)
    outs = [pltpu.make_async_copy(acc.at[pl.ds(j * half, half), :], p_out[j], tok_sem.at[0, j]) for j in range(2)]
    if bwd:
        for e in (E_RUN - 2, E_RUN - 1):
            dw_copies(dw_out, e, e % DW_SLOTS, out_sem, False)[1]()
    for c in outs:
        c.wait()


def routing_kernel(n_sub, who_ref, tab0, tab1, tab2, tab3, rank_ref, gate_ref, start_ref, nwin_ref, ntile_ref, hit_ref):
    fields, n_tok = tab0.shape
    top_k = fields // 4
    n2 = 2 * n_tok
    n_blk = n2 // 128
    r_i = lax.broadcasted_iota(i32, (128, 128), 0)
    c_i = lax.broadcasted_iota(i32, (128, 128), 1)
    tri = jnp.where(r_i <= c_i, 1.0, 0.0).astype(bf16)
    full = jnp.ones((128, 128), bf16)
    lane = lax.broadcasted_iota(i32, (2 * E_RUN, 128), 1)
    for mb in range(2):
        for q, tab in enumerate((tab0, tab1, tab2, tab3)):
            part = tab[mb * 2 * top_k:(mb + 1) * 2 * top_k, :]
            ids, gates = part[:top_k], part[top_k:]
            cols = pl.ds((q % 2) * n_tok, n_tok)
            for e in range(E_RUN):
                match = ids == who_ref[e].astype(f32)
                row = (q // 2) * E_RUN + e
                hit_ref[row:row + 1, cols] = jnp.sum(jnp.where(match, 1.0, 0.0), axis=0, keepdims=True)
                gate_ref[mb, 0, row:row + 1, cols] = jnp.sum(jnp.where(match, gates, 0.0), axis=0, keepdims=True)
        hits = [hit_ref[:, b * 128:(b + 1) * 128] for b in range(n_blk)]
        stacked = jnp.concatenate(hits, axis=0).astype(bf16)
        within = dot_nn(stacked, tri)
        totals = dot_nn(stacked, full)
        carry = jnp.zeros((2 * E_RUN, 128), f32)
        incl = []
        for b in range(n_blk):
            rows = slice(b * 2 * E_RUN, (b + 1) * 2 * E_RUN)
            v = (within[rows] + carry).astype(i32)
            rank_ref[mb, 0, :, b * 128:(b + 1) * 128] = jnp.where(hits[b] > 0.5, v - 1, -1)
            incl.append(v)
            carry = carry + totals[rows]
        for ref, fill in ((rank_ref, -1), (gate_ref, 0.0)):
            ref[mb, 1, :, :n2 - 128] = ref[mb, 0, :, ALIGN:n2 - 128 + ALIGN]
            tail = jnp.concatenate([ref[mb, 0, :, n2 - 128:], jnp.full((2 * E_RUN, 128), fill, ref.dtype)], axis=1)
            ref[mb, 1, :, n2 - 128:] = tail[:, ALIGN:128 + ALIGN]
        cnt = carry.astype(i32)

        def tokens_upto(limit):
            tot = jnp.zeros((2 * E_RUN, 128), f32)
            for v in incl:
                tot = tot + jnp.where(v <= limit, 1.0, 0.0)
            return jnp.sum(tot, axis=1, keepdims=True).astype(i32)

        start = jnp.zeros((2 * E_RUN, 128), i32)
        nwin = jnp.ones((2 * E_RUN, 128), i32)
        for j in range(n_sub):
            lo = jnp.minimum(tokens_upto(j * SUB), n2 - 1) // ALIGN * ALIGN
            hi = tokens_upto(jnp.minimum((j + 1) * SUB, cnt) - 1) + 1
            n = jnp.maximum((hi - lo - WIN + WIN_MORE - 1) // WIN_MORE, 0) + 1
            start = jnp.where(lane == j, lo, start)
            nwin = jnp.where(lane == j, n, nwin)
        start_ref[mb] = start
        nwin_ref[mb] = nwin
        tile_rows = SUB * TILE_SUBS[mb]
        ntile_ref[mb] = jnp.maximum((cnt + tile_rows - 1) // tile_rows, 1)


def run_routing(who, tables, n_sub):
    n_tok = tables[0].shape[1]
    rows = 2 * E_RUN
    wide = (2, 2, rows, 2 * n_tok)
    small = jax.ShapeDtypeStruct((2, rows, 128), i32)
    vmem = pl.BlockSpec(memory_space=pltpu.VMEM)
    return pl.pallas_call(
        functools.partial(routing_kernel, n_sub),
        out_shape=[jax.ShapeDtypeStruct(wide, i32), jax.ShapeDtypeStruct(wide, f32), small, small, small],
        in_specs=[pl.BlockSpec(memory_space=pltpu.SMEM)] + [vmem] * 4,
        out_specs=[vmem] * 5,
        scratch_shapes=[pltpu.VMEM((rows, 2 * n_tok), f32)],
        name='routing',
    )(who, *tables)


def sigmoid(v):
    return 1.0 / (1.0 + jnp.exp(-v))


def rms_scale(rows_f32):
    return lax.rsqrt(jnp.mean(rows_f32 * rows_f32, axis=-1, keepdims=True) + EPS_NORM)


def rms_back(rows_f32, cot):
    cot = cot.astype(f32)
    scale = rms_scale(rows_f32)
    proj = jnp.mean(cot * rows_f32, axis=-1, keepdims=True)
    return (scale * cot - rows_f32 * (scale * scale * scale * proj)).astype(bf16)


def dense_kernel(x_ref, w_in, w_out, norm_ref, mid_ref, *rest):
    *pre_ref, hid = rest
    x = x_ref[...].astype(f32)
    norm_in = (x * rms_scale(x)).astype(bf16)
    for c in range(0, w_in.shape[1], CHUNK):
        cols = pl.ds(c, CHUNK)
        pre = dot_nn(norm_in, w_in[:, cols]).astype(bf16)
        if pre_ref:
            pre_ref[0][:, cols] = pre
        pre = pre.astype(f32)
        hid[:, cols] = (pre * sigmoid(pre)).astype(bf16)
    mid = (x_ref[...].astype(f32) + dot_nn(hid[...], w_out[...])).astype(bf16)
    mid_ref[...] = mid
    mid = mid.astype(f32)
    norm_ref[...] = (mid * rms_scale(mid)).astype(bf16)


def run_dense(x, w_in, w_out, keep_pre):
    n_tok, width = x.shape
    ff = w_in.shape[1]
    row = pl.BlockSpec((DENSE_ROWS, width), lambda i: (i, 0))
    out_shape = [jax.ShapeDtypeStruct(x.shape, bf16)] * 2
    out_specs = [row, row]
    if keep_pre:
        out_shape += [jax.ShapeDtypeStruct((n_tok, ff), bf16)]
        out_specs += [pl.BlockSpec((DENSE_ROWS, ff), lambda i: (i, 0))]
    return pl.pallas_call(
        dense_kernel,
        grid=(n_tok // DENSE_ROWS,),
        out_shape=out_shape,
        in_specs=[row, pl.BlockSpec((width, ff), lambda i: (0, 0)), pl.BlockSpec((ff, width), lambda i: (0, 0))],
        out_specs=out_specs,
        scratch_shapes=[pltpu.VMEM((DENSE_ROWS, ff), bf16)],
        cost_estimate=pl.CostEstimate(flops=4 * n_tok * width * ff, bytes_accessed=12_000_000, transcendentals=0),
        name='dense_fwd',
    )(x, w_in, w_out)


def tail_kernel(p_own, p_mate, p_far, mid_ref, dy_ref, x_ref, pre_ref, w_in, w_out, dx_ref, d_all):
    d_norm = (p_own[...] + p_mate[...] + p_far[...]).astype(bf16)
    d_mid = (dy_ref[...].astype(f32) + rms_back(mid_ref[...].astype(f32), d_norm).astype(f32)).astype(bf16)
    for c in range(0, w_in.shape[1], CHUNK):
        cols = pl.ds(c, CHUNK)
        d_hid = dot_nt(d_mid, w_out[cols, :]).astype(bf16).astype(f32)
        pre = pre_ref[:, cols].astype(f32)
        sig = sigmoid(pre)
        d_all[:, cols] = (d_hid * (sig + pre * sig * (1.0 - sig))).astype(bf16)
    d_in = dot_nt(d_all[...], w_in[...]).astype(bf16)
    dx_ref[...] = (d_mid.astype(f32) + rms_back(x_ref[...].astype(f32), d_in).astype(f32)).astype(bf16)


def run_tail(chunk, p_own, p_mate, p_far, mid, dy, x, pre, w_in, w_out):
    n_tok, width = x.shape
    ff = w_in.shape[1]
    first, steps = TAIL[chunk], TAIL[chunk + 1] - TAIL[chunk]
    rows = n_tok // TAIL[-1]
    row = pl.BlockSpec((rows, width), lambda i: (first + i, 0))
    return pl.pallas_call(
        tail_kernel,
        grid=(steps,),
        out_shape=jax.ShapeDtypeStruct((rows * steps, width), bf16),
        in_specs=[row] * 6 + [pl.BlockSpec((rows, ff), lambda i: (first + i, 0)),
                              pl.BlockSpec((width, ff), lambda i: (0, 0)), pl.BlockSpec((ff, width), lambda i: (0, 0))],
        out_specs=pl.BlockSpec((rows, width), lambda i: (i, 0)),
        scratch_shapes=[pltpu.VMEM((rows, ff), bf16)],
        cost_estimate=pl.CostEstimate(flops=4 * rows * steps * width * ff, bytes_accessed=6_000_000, transcendentals=0),
    )(p_own, p_mate, p_far, mid, dy, x, pre, w_in, w_out)


def run_experts(meta, far, toks, dys, w_own, w_mate, dw_prev):
    starts, nwins, ntiles, base, rank, gate = meta
    bwd = dys is not None
    carry = dw_prev is not None
    half, width = toks[0].shape
    e_loc, _, ff = w_own[0].shape
    smem = pl.BlockSpec(memory_space=pltpu.SMEM)
    vmem = pl.BlockSpec(memory_space=pltpu.VMEM)
    hbm = pl.BlockSpec(memory_space=pl.ANY)
    args = [starts, nwins, ntiles, base, rank, gate, *toks]
    if bwd:
        args += [*dys]
    args += [*w_own, *w_mate]
    if carry:
        args += [*dw_prev]
    in_specs = [smem] * 4 + [vmem] * 2 + [hbm] * (len(args) - 6)
    out_shape = [jax.ShapeDtypeStruct((half, width), f32)] * 2
    if bwd:
        for n in (e_loc, 2):
            out_shape += [jax.ShapeDtypeStruct((n, *w.shape[1:]), f32) for w in w_own]
    rows = SUB * TILE_SUBS[int(bwd)]
    scratch = [
        pltpu.SMEM((E_RUN,), i32),
        pltpu.VMEM((2 * half, width), bf16),
        pltpu.VMEM((2 * half, width), f32),
        pltpu.VMEM((2, width, ff), bf16),
        pltpu.VMEM((2, width, ff), bf16),
        pltpu.VMEM((2, ff, width), bf16),
        pltpu.VMEM((rows, width), f32),
        pltpu.VMEM((rows, width), bf16),
    ]
    if bwd:
        scratch += [
            pltpu.VMEM((2 * half, width), bf16),
            pltpu.VMEM((rows, width), f32),
            pltpu.VMEM((width, rows), bf16),
            pltpu.VMEM((rows, ff), bf16),
            pltpu.VMEM((rows, ff), bf16),
            pltpu.VMEM((DW_SLOTS, width, ff), f32),
            pltpu.VMEM((DW_SLOTS, width, ff), f32),
            pltpu.VMEM((DW_SLOTS, ff, width), f32),
            pltpu.SemaphoreType.DMA((2, 2)),
            pltpu.SemaphoreType.DMA((2, 3)),
            pltpu.SemaphoreType.DMA((DW_SLOTS, 3)),
            pltpu.SemaphoreType.DMA((DW_SLOTS, 3)),
        ]
    else:
        scratch += [
            pltpu.VMEM((rows, ff), bf16),
            pltpu.SemaphoreType.DMA((2, 2)),
            pltpu.SemaphoreType.DMA((2, 3)),
        ]
    flops = (8 if bwd else 3) * 2 * 3584 * 2 * width * ff
    return pl.pallas_call(
        functools.partial(expert_kernel, bwd, carry, E_RUN if far else 0),
        out_shape=out_shape,
        in_specs=in_specs,
        out_specs=[hbm] * len(out_shape),
        scratch_shapes=scratch,
        compiler_params=pltpu.CompilerParams(vmem_limit_bytes=60 * 1024 * 1024),
        cost_estimate=pl.CostEstimate(flops=flops, bytes_accessed=60_000_000, transcendentals=0),
        name='experts_bwd' if bwd else 'experts_fwd',
    )(*args)


def solution(mesh):
    n_ep = mesh.shape['ep']
    n_pp = mesh.shape['pp']
    n_tail = len(TAIL) - 1
    fwd_perm = [(i, (i + 1) % n_pp) for i in range(n_pp)]
    bwd_perm = [(i, (i - 1) % n_pp) for i in range(n_pp)]

    def to_mate(v):
        return lax.ppermute(v, 'ep', [(i, i ^ 1) for i in range(n_ep)])

    def to_cross(v):
        return lax.ppermute(v, 'ep', [(i, i ^ 2) for i in range(n_ep)])

    def device_fn(x_fwd, x_bwd, dy_bwd, ids_fwd, gate_fwd, ids_bwd, gate_bwd, w_in, w_out, w_gate, w_up, w_down):
        fwd_x, bwd_x, bwd_dy = x_fwd[0], x_bwd[0], dy_bwd[0]
        stage_w_in, stage_w_out = w_in[0], w_out[0]
        w_own = (w_gate[0], w_up[0], w_down[0])
        n_tok, _ = fwd_x.shape
        top_k = ids_fwd.shape[2]
        e_loc = w_own[0].shape[0]
        n_exp = e_loc * n_ep
        cap = 3 * n_tok * top_k // n_exp
        me = lax.axis_index('ep')
        core = lax.rem(me, 2)
        base = 2 * core
        n_sub = -(-2 * cap // SUB)

        def gather_pair(v):
            far = to_cross(v)
            return (v, to_mate(v)), (far, to_mate(far))

        fields = [ids_fwd[0].astype(f32).T, gate_fwd[0].astype(f32).T, ids_bwd[0].astype(f32).T, gate_bwd[0].astype(f32).T]
        table = jnp.concatenate(fields)
        tables = [table, to_mate(table), to_cross(table)]
        tables.append(lax.ppermute(table, 'ep', [(i, i ^ 3) for i in range(n_ep)]))
        mine = e_loc * me + base
        mates = e_loc * (me ^ 1) + base
        who = jnp.stack([mine, mine + 1, mates, mates + 1]).astype(i32)
        base_arr = base.reshape(1).astype(i32)
        ranks, gates, starts, nwins, ntiles = run_routing(who, tables, n_sub)
        meta = (starts, nwins, ntiles, base_arr, ranks, gates)

        far_dy = to_cross(bwd_dy)
        dy_near, dy_far = (bwd_dy, to_mate(bwd_dy)), (far_dy, to_mate(far_dy))
        w_mate = tuple(to_mate(w) for w in w_own)

        def combine(parts):
            return parts[0] + to_mate(parts[1])

        norm_f, mid_f = run_dense(fwd_x, stage_w_in, stage_w_out, False)
        near_f, far_f = gather_pair(norm_f)
        norm_b, mid_b, pre_b = run_dense(bwd_x, stage_w_in, stage_w_out, True)
        near_b, far_b = gather_pair(norm_b)

        pf_near = run_experts(meta, False, near_f, None, w_own, w_mate, None)
        pf_far = run_experts(meta, True, far_f, None, w_own, w_mate, None)
        ret_f = to_cross(combine(pf_far))
        pb_far = run_experts(meta, True, far_b, dy_far, w_own, w_mate, None)
        ret_b = to_cross(combine(pb_far[:2]))
        pb_near = run_experts(meta, False, near_b, dy_near, w_own, w_mate, pb_far[2:])
        dw_full, dw_mate = pb_near[2:5], pb_near[5:8]

        near_f_mate = to_mate(pf_near[1])
        y_val = (mid_f.astype(f32) + (pf_near[0] + near_f_mate + ret_f)).astype(bf16)
        y_next = lax.ppermute(y_val, 'pp', fwd_perm)

        dx_parts = []
        from_mate = to_mate(pb_near[1])
        for c in range(n_tail):
            dx_val = run_tail(c, pb_near[0], from_mate, ret_b, mid_b, bwd_dy, bwd_x, pre_b, stage_w_in, stage_w_out)
            dx_parts.append(lax.ppermute(dx_val, 'pp', bwd_perm))
        dx_prev = jnp.concatenate(dx_parts)

        back = [to_mate(v) for v in dw_mate]
        zero = jnp.zeros((), i32)
        dw_gate, dw_up, dw_down = [lax.dynamic_update_slice(full, part, (2 - base, zero, zero)) for full, part in zip(dw_full, back)]
        return y_next[None], dx_prev[None], dw_gate[None], dw_up[None], dw_down[None]

    spec_act = P('pp', 'ep', None)
    spec_dense = P('pp', None, None)
    spec_exp = P('pp', 'ep', None, None)


    return jax.shard_map(device_fn, mesh=mesh, in_specs=(spec_act,) * 7 + (spec_dense,) * 2 + (spec_exp,) * 3, out_specs=(spec_act, spec_act, spec_exp, spec_exp, spec_exp), check_vma=False)
```

```python
import functools

import jax
import jax.numpy as jnp
from jax import lax
from jax.experimental import pallas as pl
from jax.experimental.pallas import tpu as pltpu
from jax.sharding import PartitionSpec as P


EPS_NORM = 1e-6
SUB = 128
TILE_SUBS = (3, 4)
WIN = 256
WIN_MORE = 1536
ALIGN = 64
CHUNK = 256
OUT_ROWS = 256
DW_SLOTS = 3
TAIL = (0, 1, 3, 5, 8)
DENSE_ROWS = 512
E_RUN = 4

f32 = jnp.float32
bf16 = jnp.bfloat16
i32 = jnp.int32


def dot_nn(a, b):
    return lax.dot_general(a, b, (((1,), (0,)), ((), ())), preferred_element_type=f32)


def dot_nt(a, b):
    return lax.dot_general(a, b, (((1,), (1,)), ((), ())), preferred_element_type=f32)


def dot_tn(a, b):
    return lax.dot_general(a, b, (((0,), (0,)), ((), ())), preferred_element_type=f32)


def expert_kernel(bwd, carry, row0, n_out, *refs):
    refs = list(refs)

    def take(n):
        out = refs[:n]
        del refs[:n]
        return out

    starts, nwins, ntiles, base_ref, rank_ref, gate_ref = take(6)
    tok_in = take(2)
    dy_in = take(2) if bwd else []
    mb = int(bwd)
    per_tile = TILE_SUBS[mb]
    w_own = take(3)
    w_mate = take(3)
    dw_in = take(6) if carry else []
    p_out = take(n_out)
    dw_out = take(6) if bwd else []
    order, tok, acc, wg_buf, wu_buf, wd_buf, x_acc, out_all = take(8)
    if bwd:
        dyt, d_acc, xt, dg_all, du_all, dwg_buf, dwu_buf, dwd_buf = take(8)
        tok_sem, w_sem, p_sem, in_sem, out_sem = take(5)
    else:
        (act_all,) = take(1)
        tok_sem, w_sem, p_sem = take(3)
    half = tok_in[0].shape[0]
    n_tok = 2 * half
    ff = wg_buf.shape[2]
    base = base_ref[0]

    loads = []
    for i, (src, dst) in enumerate([(tok_in, tok)] + ([(dy_in, dyt)] if bwd else [])):
        for j in range(2):
            loads.append(pltpu.make_async_copy(src[j], dst.at[pl.ds(j * half, half), :], tok_sem.at[i, j]))
    for c in loads:
        c.start()

    def w_copies(srcs, idx, slot):
        return [pltpu.make_async_copy(s.at[idx], b.at[slot], w_sem.at[slot, k])
                for k, (s, b) in enumerate(zip(srcs, (wg_buf, wu_buf, wd_buf)))]

    def w_start(e, slot):
        @pl.when(e < 2)
        def _():
            for c in w_copies(w_own, base + e, slot):
                c.start()

        @pl.when(e >= 2)
        def _():
            for c in w_copies(w_mate, base + e - 2, slot):
                c.start()

    def dw_copies(refs6, e, slot, sem, inward):
        bufs = (dwg_buf, dwu_buf, dwd_buf)

        def go(refs3, idx, what):
            for k in range(3):
                hbm, buf = refs3[k].at[idx], bufs[k].at[slot]
                c = pltpu.make_async_copy(hbm, buf, sem.at[slot, k]) if inward else pltpu.make_async_copy(buf, hbm, sem.at[slot, k])
                getattr(c, what)()

        def start():
            @pl.when(e < 2)
            def _():
                go(refs6[:3], base + e, 'start')

            @pl.when(e >= 2)
            def _():
                go(refs6[3:], e - 2, 'start')

        def wait():
            go(refs6[3:], 0, 'wait')

        return start, wait

    tiles_of = [ntiles[mb, row0 + e, 0] for e in range(E_RUN)]
    for e in range(E_RUN):
        rank = 0
        for o in range(E_RUN):
            if o != e:
                ahead = tiles_of[o] >= tiles_of[e] if o < e else tiles_of[o] > tiles_of[e]
                rank = rank + ahead.astype(i32)
        place = jnp.where(rank == 0, 0, jnp.where(rank == 1, E_RUN - 1, rank - 1))
        order[place] = e

    def clear(ref):
        rows = 64

        @pl.loop(0, ref.shape[0] // rows)
        def _(k):
            ref[pl.ds(pl.multiple_of(k * rows, rows), rows), :] = jnp.zeros((rows, ref.shape[1]), ref.dtype)

    w_start(order[0], 0)
    if carry:
        dw_copies(dw_in, order[0], 0, in_sem, True)[0]()
    clear(acc)
    for c in loads:
        c.wait()

    def window(e, st, k):
        size = WIN_MORE if k is not None else WIN
        so = starts[mb, row0 + e, st]
        if k is not None:
            so += WIN + (k - 1) * WIN_MORE
        s = jnp.minimum(so, n_tok - size)
        shift = lax.rem(s // ALIGN, 2)
        lanes = pl.ds(pl.multiple_of(s - shift * ALIGN, 128), size)
        rk = rank_ref[mb, shift, pl.ds(row0 + e, 1), lanes]
        lane = lax.broadcasted_iota(i32, (1, size), 1) + s
        rk = jnp.where(lane >= so, rk, -1) - st * SUB
        mask = lax.broadcasted_iota(i32, (SUB, size), 0) == rk
        toks = pl.ds(pl.multiple_of(s, ALIGN), size)
        return toks, lambda: jnp.where(mask, 1.0, 0.0).astype(bf16), \
            lambda: jnp.where(mask, gate_ref[mb, shift, pl.ds(row0 + e, 1), lanes], 0.0).astype(bf16)

    bounds = [0]
    for ref in p_out:
        bounds.append(bounds[-1] + ref.shape[0])

    def p_copy(q):
        for j, dst in enumerate(p_out):
            lo, hi = bounds[j] // OUT_ROWS, bounds[j + 1] // OUT_ROWS

            @pl.when((q >= lo) & (q < hi))
            def _():
                rows = pl.ds(pl.multiple_of((q - lo) * OUT_ROWS, OUT_ROWS), OUT_ROWS)
                src = acc.at[pl.ds(pl.multiple_of(q * OUT_ROWS, OUT_ROWS), OUT_ROWS), :]
                pltpu.make_async_copy(src, dst.at[rows, :], p_sem.at[j]).start()

    def expert(i, _):
        e = order[i]
        slot = lax.rem(i, 2)
        for c in w_copies(w_own, 0, slot):
            c.wait()

        @pl.when(i < E_RUN - 1)
        def _():
            w_start(order[i + 1], 1 - slot)

        wg, wu, wd = wg_buf.at[slot], wu_buf.at[slot], wd_buf.at[slot]
        if bwd:
            d_slot = lax.rem(i, DW_SLOTS)

            @pl.when(i >= 2)
            def _():
                dw_copies(dw_out, 0, lax.rem(i - 2, DW_SLOTS), out_sem, False)[1]()

            if carry:
                @pl.when(i < E_RUN - 1)
                def _():
                    dw_copies(dw_in, order[i + 1], lax.rem(i + 1, DW_SLOTS), in_sem, True)[0]()

                dw_copies(dw_in, e, d_slot, in_sem, True)[1]()
            else:
                for b in (dwg_buf, dwu_buf, dwd_buf):
                    clear(b.at[d_slot])
            dwg, dwu, dwd = dwg_buf.at[d_slot], dwu_buf.at[d_slot], dwd_buf.at[d_slot]

        def tile(t, _):
            for h in range(per_tile):
                rows = pl.ds(h * SUB, SUB)
                toks, ones, gated = window(e, t * per_tile + h, None)
                x_acc[rows, :] = dot_nn(ones(), tok[toks, :])
                if bwd:
                    d_acc[rows, :] = dot_nn(gated(), dyt[toks, :])

            n_win = nwins[mb, row0 + e, t * per_tile]
            for h in range(1, per_tile):
                n_win = jnp.maximum(n_win, nwins[mb, row0 + e, t * per_tile + h])

            @pl.when(n_win > 1)
            def _():
                @pl.loop(0, per_tile)
                def _(h):
                    st = t * per_tile + h
                    rows = pl.ds(pl.multiple_of(h * SUB, SUB), SUB)

                    @pl.loop(1, nwins[mb, row0 + e, st])
                    def _(k):
                        toks, ones, gated = window(e, st, k)
                        x_acc[rows, :] += dot_nn(ones(), tok[toks, :])
                        if bwd:
                            d_acc[rows, :] += dot_nn(gated(), dyt[toks, :])

            x = x_acc[...].astype(bf16)
            if bwd:
                d = d_acc[...].astype(bf16)
                xt[...] = x.T
            for c in range(0, ff, CHUNK):
                cols = pl.ds(c, CHUNK)
                gp = dot_nn(x, wg[:, cols]).astype(bf16).astype(f32)
                up = dot_nn(x, wu[:, cols]).astype(bf16).astype(f32)
                sig = 1.0 / (1.0 + jnp.exp(-gp))
                silu = gp * sig
                if not bwd:
                    act_all[:, cols] = (silu * up).astype(bf16)
                    continue
                da = dot_nt(d, wd[cols, :]).astype(bf16).astype(f32)
                act = (silu * up).astype(bf16)
                du = (da * silu).astype(bf16)
                dg = (da * up * (sig + silu * (1.0 - sig))).astype(bf16)
                dg_all[:, cols] = dg
                du_all[:, cols] = du
                dwd[cols, :] += dot_tn(act, d)
                dwg[:, cols] += dot_nn(xt[...], dg)
                dwu[:, cols] += dot_nn(xt[...], du)
            if bwd:
                out = (dot_nt(dg_all[...], wg[...]) + dot_nt(du_all[...], wu[...])).astype(bf16)
            else:
                out = dot_nn(act_all[...], wd[...]).astype(bf16)

            def put(st, k, part):
                toks, ones, gated = window(e, st, k)
                acc[toks, :] += dot_tn(ones() if bwd else gated(), part)

            out_all[...] = out
            for h in range(per_tile):
                put(t * per_tile + h, None, out[h * SUB:(h + 1) * SUB, :])

            @pl.when(n_win > 1)
            def _():
                @pl.loop(0, per_tile)
                def _(h):
                    st = t * per_tile + h

                    @pl.loop(1, nwins[mb, row0 + e, st])
                    def _(k):
                        put(st, k, out_all[pl.ds(pl.multiple_of(h * SUB, SUB), SUB), :])

            @pl.when(i == E_RUN - 1)
            def _():
                def final(tile_idx):
                    return jnp.minimum(starts[mb, row0 + e, tile_idx * per_tile], n_tok - WIN_MORE) // OUT_ROWS

                lo = jnp.where(t == 0, 0, final(t))
                hi = jnp.where(t == ntiles[mb, row0 + e, 0] - 1, n_tok // OUT_ROWS, final(t + 1))

                @pl.loop(lo, hi)
                def _(q):
                    p_copy(q)

            return 0

        lax.fori_loop(0, ntiles[mb, row0 + e, 0], tile, 0)
        if bwd:
            dw_copies(dw_out, e, d_slot, out_sem, False)[0]()
        return 0

    lax.fori_loop(0, E_RUN, expert, 0)
    outs = [pltpu.make_async_copy(acc.at[pl.ds(bounds[j], ref.shape[0]), :], ref, p_sem.at[j]) for j, ref in enumerate(p_out)]
    if bwd:
        for e in (E_RUN - 2, E_RUN - 1):
            dw_copies(dw_out, e, e % DW_SLOTS, out_sem, False)[1]()
    for c in outs:
        c.wait()


def routing_kernel(n_sub, who_ref, tab0, tab1, tab2, tab3, rank_ref, gate_ref, start_ref, nwin_ref, ntile_ref, hit_ref):
    fields, n_tok = tab0.shape
    top_k = fields // 4
    n2 = 2 * n_tok
    n_blk = n2 // 128
    r_i = lax.broadcasted_iota(i32, (128, 128), 0)
    c_i = lax.broadcasted_iota(i32, (128, 128), 1)
    tri = jnp.where(r_i <= c_i, 1.0, 0.0).astype(bf16)
    full = jnp.ones((128, 128), bf16)
    lane = lax.broadcasted_iota(i32, (2 * E_RUN, 128), 1)
    for mb in range(2):
        for q, tab in enumerate((tab0, tab1, tab2, tab3)):
            part = tab[mb * 2 * top_k:(mb + 1) * 2 * top_k, :]
            ids, gates = part[:top_k], part[top_k:]
            cols = pl.ds((q % 2) * n_tok, n_tok)
            for e in range(E_RUN):
                match = ids == who_ref[e].astype(f32)
                row = (q // 2) * E_RUN + e
                hit_ref[row:row + 1, cols] = jnp.sum(jnp.where(match, 1.0, 0.0), axis=0, keepdims=True)
                gate_ref[mb, 0, row:row + 1, cols] = jnp.sum(jnp.where(match, gates, 0.0), axis=0, keepdims=True)
        hits = [hit_ref[:, b * 128:(b + 1) * 128] for b in range(n_blk)]
        stacked = jnp.concatenate(hits, axis=0).astype(bf16)
        within = dot_nn(stacked, tri)
        totals = dot_nn(stacked, full)
        carry = jnp.zeros((2 * E_RUN, 128), f32)
        incl = []
        for b in range(n_blk):
            rows = slice(b * 2 * E_RUN, (b + 1) * 2 * E_RUN)
            v = (within[rows] + carry).astype(i32)
            rank_ref[mb, 0, :, b * 128:(b + 1) * 128] = jnp.where(hits[b] > 0.5, v - 1, -1)
            incl.append(v)
            carry = carry + totals[rows]
        for ref, fill in ((rank_ref, -1), (gate_ref, 0.0)):
            ref[mb, 1, :, :n2 - 128] = ref[mb, 0, :, ALIGN:n2 - 128 + ALIGN]
            tail = jnp.concatenate([ref[mb, 0, :, n2 - 128:], jnp.full((2 * E_RUN, 128), fill, ref.dtype)], axis=1)
            ref[mb, 1, :, n2 - 128:] = tail[:, ALIGN:128 + ALIGN]
        cnt = carry.astype(i32)

        def tokens_upto(limit):
            tot = jnp.zeros((2 * E_RUN, 128), f32)
            for v in incl:
                tot = tot + jnp.where(v <= limit, 1.0, 0.0)
            return jnp.sum(tot, axis=1, keepdims=True).astype(i32)

        start = jnp.zeros((2 * E_RUN, 128), i32)
        nwin = jnp.ones((2 * E_RUN, 128), i32)
        for j in range(n_sub):
            lo = jnp.minimum(tokens_upto(j * SUB), n2 - 1) // ALIGN * ALIGN
            hi = tokens_upto(jnp.minimum((j + 1) * SUB, cnt) - 1) + 1
            n = jnp.maximum((hi - lo - WIN + WIN_MORE - 1) // WIN_MORE, 0) + 1
            start = jnp.where(lane == j, lo, start)
            nwin = jnp.where(lane == j, n, nwin)
        start_ref[mb] = start
        nwin_ref[mb] = nwin
        tile_rows = SUB * TILE_SUBS[mb]
        ntile_ref[mb] = jnp.maximum((cnt + tile_rows - 1) // tile_rows, 1)


def run_routing(who, tables, n_sub):
    n_tok = tables[0].shape[1]
    rows = 2 * E_RUN
    wide = (2, 2, rows, 2 * n_tok)
    small = jax.ShapeDtypeStruct((2, rows, 128), i32)
    vmem = pl.BlockSpec(memory_space=pltpu.VMEM)
    return pl.pallas_call(
        functools.partial(routing_kernel, n_sub),
        out_shape=[jax.ShapeDtypeStruct(wide, i32), jax.ShapeDtypeStruct(wide, f32), small, small, small],
        in_specs=[pl.BlockSpec(memory_space=pltpu.SMEM)] + [vmem] * 4,
        out_specs=[vmem] * 5,
        scratch_shapes=[pltpu.VMEM((rows, 2 * n_tok), f32)],
        name='routing',
    )(who, *tables)


def sigmoid(v):
    return 1.0 / (1.0 + jnp.exp(-v))


def rms_scale(rows_f32):
    return lax.rsqrt(jnp.mean(rows_f32 * rows_f32, axis=-1, keepdims=True) + EPS_NORM)


def rms_back(rows_f32, cot):
    cot = cot.astype(f32)
    scale = rms_scale(rows_f32)
    proj = jnp.mean(cot * rows_f32, axis=-1, keepdims=True)
    return (scale * cot - rows_f32 * (scale * scale * scale * proj)).astype(bf16)


def dense_kernel(x_ref, w_in, w_out, norm_ref, mid_ref, *rest):
    *pre_ref, hid = rest
    x = x_ref[...].astype(f32)
    norm_in = (x * rms_scale(x)).astype(bf16)
    for c in range(0, w_in.shape[1], CHUNK):
        cols = pl.ds(c, CHUNK)
        pre = dot_nn(norm_in, w_in[:, cols]).astype(bf16)
        if pre_ref:
            pre_ref[0][:, cols] = pre
        pre = pre.astype(f32)
        hid[:, cols] = (pre * sigmoid(pre)).astype(bf16)
    mid = (x_ref[...].astype(f32) + dot_nn(hid[...], w_out[...])).astype(bf16)
    mid_ref[...] = mid
    mid = mid.astype(f32)
    norm_ref[...] = (mid * rms_scale(mid)).astype(bf16)


def run_dense(x, w_in, w_out, keep_pre):
    n_tok, width = x.shape
    ff = w_in.shape[1]
    row = pl.BlockSpec((DENSE_ROWS, width), lambda i: (i, 0))
    out_shape = [jax.ShapeDtypeStruct(x.shape, bf16)] * 2
    out_specs = [row, row]
    if keep_pre:
        out_shape += [jax.ShapeDtypeStruct((n_tok, ff), bf16)]
        out_specs += [pl.BlockSpec((DENSE_ROWS, ff), lambda i: (i, 0))]
    return pl.pallas_call(
        dense_kernel,
        grid=(n_tok // DENSE_ROWS,),
        out_shape=out_shape,
        in_specs=[row, pl.BlockSpec((width, ff), lambda i: (0, 0)), pl.BlockSpec((ff, width), lambda i: (0, 0))],
        out_specs=out_specs,
        scratch_shapes=[pltpu.VMEM((DENSE_ROWS, ff), bf16)],
        cost_estimate=pl.CostEstimate(flops=4 * n_tok * width * ff, bytes_accessed=12_000_000, transcendentals=0),
        name='dense_fwd',
    )(x, w_in, w_out)


def tail_kernel(p_own, p_mate, p_far, mid_ref, dy_ref, x_ref, pre_ref, w_in, w_out, dx_ref, d_all):
    d_norm = (p_own[...] + p_mate[...] + p_far[...]).astype(bf16)
    d_mid = (dy_ref[...].astype(f32) + rms_back(mid_ref[...].astype(f32), d_norm).astype(f32)).astype(bf16)
    for c in range(0, w_in.shape[1], CHUNK):
        cols = pl.ds(c, CHUNK)
        d_hid = dot_nt(d_mid, w_out[cols, :]).astype(bf16).astype(f32)
        pre = pre_ref[:, cols].astype(f32)
        sig = sigmoid(pre)
        d_all[:, cols] = (d_hid * (sig + pre * sig * (1.0 - sig))).astype(bf16)
    d_in = dot_nt(d_all[...], w_in[...]).astype(bf16)
    dx_ref[...] = (d_mid.astype(f32) + rms_back(x_ref[...].astype(f32), d_in).astype(f32)).astype(bf16)


def run_tail(chunk, p_own, p_mate, p_far, mid, dy, x, pre, w_in, w_out):
    n_tok, width = x.shape
    ff = w_in.shape[1]
    first, steps = TAIL[chunk], TAIL[chunk + 1] - TAIL[chunk]
    rows = n_tok // TAIL[-1]
    row = pl.BlockSpec((rows, width), lambda i: (first + i, 0))
    return pl.pallas_call(
        tail_kernel,
        grid=(steps,),
        out_shape=jax.ShapeDtypeStruct((rows * steps, width), bf16),
        in_specs=[row, pl.BlockSpec((rows, width), lambda i: (first + i if chunk == 0 else first + i - 1, 0))] + [row] * 4 + [pl.BlockSpec((rows, ff), lambda i: (first + i, 0)),
                              pl.BlockSpec((width, ff), lambda i: (0, 0)), pl.BlockSpec((ff, width), lambda i: (0, 0))],
        out_specs=pl.BlockSpec((rows, width), lambda i: (i, 0)),
        scratch_shapes=[pltpu.VMEM((rows, ff), bf16)],
        cost_estimate=pl.CostEstimate(flops=4 * rows * steps * width * ff, bytes_accessed=6_000_000, transcendentals=0),
    )(p_own, p_mate, p_far, mid, dy, x, pre, w_in, w_out)


def run_experts(meta, far, toks, dys, w_own, w_mate, dw_prev):
    starts, nwins, ntiles, base, rank, gate = meta
    bwd = dys is not None
    carry = dw_prev is not None
    half, width = toks[0].shape
    e_loc, _, ff = w_own[0].shape
    smem = pl.BlockSpec(memory_space=pltpu.SMEM)
    vmem = pl.BlockSpec(memory_space=pltpu.VMEM)
    hbm = pl.BlockSpec(memory_space=pl.ANY)
    args = [starts, nwins, ntiles, base, rank, gate, *toks]
    if bwd:
        args += [*dys]
    args += [*w_own, *w_mate]
    if carry:
        args += [*dw_prev]
    in_specs = [smem] * 4 + [vmem] * 2 + [hbm] * (len(args) - 6)
    p_rows = [half, OUT_ROWS, half - OUT_ROWS] if carry else [half, half]
    out_shape = [jax.ShapeDtypeStruct((n, width), f32) for n in p_rows]
    if bwd:
        for n in (e_loc, 2):
            out_shape += [jax.ShapeDtypeStruct((n, *w.shape[1:]), f32) for w in w_own]
    rows = SUB * TILE_SUBS[int(bwd)]
    scratch = [
        pltpu.SMEM((E_RUN,), i32),
        pltpu.VMEM((2 * half, width), bf16),
        pltpu.VMEM((2 * half, width), f32),
        pltpu.VMEM((2, width, ff), bf16),
        pltpu.VMEM((2, width, ff), bf16),
        pltpu.VMEM((2, ff, width), bf16),
        pltpu.VMEM((rows, width), f32),
        pltpu.VMEM((rows, width), bf16),
    ]
    if bwd:
        scratch += [
            pltpu.VMEM((2 * half, width), bf16),
            pltpu.VMEM((rows, width), f32),
            pltpu.VMEM((width, rows), bf16),
            pltpu.VMEM((rows, ff), bf16),
            pltpu.VMEM((rows, ff), bf16),
            pltpu.VMEM((DW_SLOTS, width, ff), f32),
            pltpu.VMEM((DW_SLOTS, width, ff), f32),
            pltpu.VMEM((DW_SLOTS, ff, width), f32),
            pltpu.SemaphoreType.DMA((2, 2)),
            pltpu.SemaphoreType.DMA((2, 3)),
            pltpu.SemaphoreType.DMA((3,)),
            pltpu.SemaphoreType.DMA((DW_SLOTS, 3)),
            pltpu.SemaphoreType.DMA((DW_SLOTS, 3)),
        ]
    else:
        scratch += [
            pltpu.VMEM((rows, ff), bf16),
            pltpu.SemaphoreType.DMA((2, 2)),
            pltpu.SemaphoreType.DMA((2, 3)),
            pltpu.SemaphoreType.DMA((3,)),
        ]
    flops = (8 if bwd else 3) * 2 * 3584 * 2 * width * ff
    return pl.pallas_call(
        functools.partial(expert_kernel, bwd, carry, E_RUN if far else 0, len(p_rows)),
        out_shape=out_shape,
        in_specs=in_specs,
        out_specs=[hbm] * len(out_shape),
        scratch_shapes=scratch,
        compiler_params=pltpu.CompilerParams(vmem_limit_bytes=60 * 1024 * 1024),
        cost_estimate=pl.CostEstimate(flops=flops, bytes_accessed=60_000_000, transcendentals=0),
        name='experts_bwd' if bwd else 'experts_fwd',
    )(*args)


def solution(mesh):
    n_ep = mesh.shape['ep']
    n_pp = mesh.shape['pp']
    n_tail = len(TAIL) - 1
    fwd_perm = [(i, (i + 1) % n_pp) for i in range(n_pp)]
    bwd_perm = [(i, (i - 1) % n_pp) for i in range(n_pp)]

    def to_mate(v):
        return lax.ppermute(v, 'ep', [(i, i ^ 1) for i in range(n_ep)])

    def to_cross(v):
        return lax.ppermute(v, 'ep', [(i, i ^ 2) for i in range(n_ep)])

    def device_fn(x_fwd, x_bwd, dy_bwd, ids_fwd, gate_fwd, ids_bwd, gate_bwd, w_in, w_out, w_gate, w_up, w_down):
        fwd_x, bwd_x, bwd_dy = x_fwd[0], x_bwd[0], dy_bwd[0]
        stage_w_in, stage_w_out = w_in[0], w_out[0]
        w_own = (w_gate[0], w_up[0], w_down[0])
        n_tok, _ = fwd_x.shape
        top_k = ids_fwd.shape[2]
        e_loc = w_own[0].shape[0]
        n_exp = e_loc * n_ep
        cap = 3 * n_tok * top_k // n_exp
        me = lax.axis_index('ep')
        core = lax.rem(me, 2)
        base = 2 * core
        n_sub = -(-2 * cap // SUB)

        def gather_pair(v):
            far = to_cross(v)
            return (v, to_mate(v)), (far, to_mate(far))

        fields = [ids_fwd[0].astype(f32).T, gate_fwd[0].astype(f32).T, ids_bwd[0].astype(f32).T, gate_bwd[0].astype(f32).T]
        table = jnp.concatenate(fields)
        tables = [table, to_mate(table), to_cross(table)]
        tables.append(lax.ppermute(table, 'ep', [(i, i ^ 3) for i in range(n_ep)]))
        mine = e_loc * me + base
        mates = e_loc * (me ^ 1) + base
        who = jnp.stack([mine, mine + 1, mates, mates + 1]).astype(i32)
        base_arr = base.reshape(1).astype(i32)
        ranks, gates, starts, nwins, ntiles = run_routing(who, tables, n_sub)
        meta = (starts, nwins, ntiles, base_arr, ranks, gates)

        far_dy = to_cross(bwd_dy)
        dy_near, dy_far = (bwd_dy, to_mate(bwd_dy)), (far_dy, to_mate(far_dy))
        w_mate = tuple(to_mate(w) for w in w_own)

        def combine(parts):
            return parts[0] + to_mate(parts[1])

        norm_f, mid_f = run_dense(fwd_x, stage_w_in, stage_w_out, False)
        near_f, far_f = gather_pair(norm_f)
        norm_b, mid_b, pre_b = run_dense(bwd_x, stage_w_in, stage_w_out, True)
        near_b, far_b = gather_pair(norm_b)

        pf_near = run_experts(meta, False, near_f, None, w_own, w_mate, None)
        pf_far = run_experts(meta, True, far_f, None, w_own, w_mate, None)
        ret_f = to_cross(combine(pf_far))
        pb_far = run_experts(meta, True, far_b, dy_far, w_own, w_mate, None)
        ret_b = to_cross(combine(pb_far[:2]))
        pb_near = run_experts(meta, False, near_b, dy_near, w_own, w_mate, pb_far[2:])
        dw_full, dw_mate = pb_near[3:6], pb_near[6:9]

        near_f_mate = to_mate(pf_near[1])
        y_val = (mid_f.astype(f32) + (pf_near[0] + near_f_mate + ret_f)).astype(bf16)
        y_next = lax.ppermute(y_val, 'pp', fwd_perm)

        dx_parts = []
        from_mate = [to_mate(pb_near[1 + k]) for k in range(2)]
        for c in range(n_tail):
            dx_val = run_tail(c, pb_near[0], from_mate[min(c, 1)], ret_b, mid_b, bwd_dy, bwd_x, pre_b, stage_w_in, stage_w_out)
            dx_parts.append(lax.ppermute(dx_val, 'pp', bwd_perm))
        dx_prev = jnp.concatenate(dx_parts)

        back = [to_mate(v) for v in dw_mate]
        zero = jnp.zeros((), i32)
        dw_gate, dw_up, dw_down = [lax.dynamic_update_slice(full, part, (2 - base, zero, zero)) for full, part in zip(dw_full, back)]
        return y_next[None], dx_prev[None], dw_gate[None], dw_up[None], dw_down[None]

    spec_act = P('pp', 'ep', None)
    spec_dense = P('pp', None, None)
    spec_exp = P('pp', 'ep', None, None)


    return jax.shard_map(device_fn, mesh=mesh, in_specs=(spec_act,) * 7 + (spec_dense,) * 2 + (spec_exp,) * 3, out_specs=(spec_act, spec_act, spec_exp, spec_exp, spec_exp), check_vma=False)
```

```python
import functools

import jax
import jax.numpy as jnp
from jax import lax
from jax.experimental import pallas as pl
from jax.experimental.pallas import tpu as pltpu
from jax.sharding import PartitionSpec as P


EPS_NORM = 1e-6
SUB = 128
TILE_SUBS = (3, 4)
WIN = 256
WIN_MORE = 1536
ALIGN = 64
CHUNK = 256
OUT_ROWS = 256
DW_SLOTS = 3
TAIL = (0, 2, 6, 10, 16)
DENSE_ROWS = 256
E_RUN = 4

f32 = jnp.float32
bf16 = jnp.bfloat16
i32 = jnp.int32


def dot_nn(a, b):
    return lax.dot_general(a, b, (((1,), (0,)), ((), ())), preferred_element_type=f32)


def dot_nt(a, b):
    return lax.dot_general(a, b, (((1,), (1,)), ((), ())), preferred_element_type=f32)


def dot_tn(a, b):
    return lax.dot_general(a, b, (((0,), (0,)), ((), ())), preferred_element_type=f32)


def expert_kernel(bwd, carry, row0, n_out, *refs):
    refs = list(refs)

    def take(n):
        out = refs[:n]
        del refs[:n]
        return out

    starts, nwins, ntiles, base_ref, rank_ref, gate_ref = take(6)
    tok_in = take(2)
    dy_in = take(2) if bwd else []
    mb = int(bwd)
    per_tile = TILE_SUBS[mb]
    w_own = take(3)
    w_mate = take(3)
    dw_in = take(6) if carry else []
    p_out = take(n_out)
    dw_out = take(6) if bwd else []
    order, tok, acc, wg_buf, wu_buf, wd_buf, x_acc, out_all = take(8)
    if bwd:
        dyt, d_acc, xt, dg_all, du_all, dwg_buf, dwu_buf, dwd_buf = take(8)
        tok_sem, w_sem, p_sem, in_sem, out_sem = take(5)
    else:
        (act_all,) = take(1)
        tok_sem, w_sem, p_sem = take(3)
    half = tok_in[0].shape[0]
    n_tok = 2 * half
    ff = wg_buf.shape[2]
    base = base_ref[0]

    loads = []
    for i, (src, dst) in enumerate([(tok_in, tok)] + ([(dy_in, dyt)] if bwd else [])):
        for j in range(2):
            loads.append(pltpu.make_async_copy(src[j], dst.at[pl.ds(j * half, half), :], tok_sem.at[i, j]))
    for c in loads:
        c.start()

    def w_copies(srcs, idx, slot):
        return [pltpu.make_async_copy(s.at[idx], b.at[slot], w_sem.at[slot, k])
                for k, (s, b) in enumerate(zip(srcs, (wg_buf, wu_buf, wd_buf)))]

    def w_start(e, slot):
        @pl.when(e < 2)
        def _():
            for c in w_copies(w_own, base + e, slot):
                c.start()

        @pl.when(e >= 2)
        def _():
            for c in w_copies(w_mate, base + e - 2, slot):
                c.start()

    def dw_copies(refs6, e, slot, sem, inward):
        bufs = (dwg_buf, dwu_buf, dwd_buf)

        def go(refs3, idx, what):
            for k in range(3):
                hbm, buf = refs3[k].at[idx], bufs[k].at[slot]
                c = pltpu.make_async_copy(hbm, buf, sem.at[slot, k]) if inward else pltpu.make_async_copy(buf, hbm, sem.at[slot, k])
                getattr(c, what)()

        def start():
            @pl.when(e < 2)
            def _():
                go(refs6[:3], base + e, 'start')

            @pl.when(e >= 2)
            def _():
                go(refs6[3:], e - 2, 'start')

        def wait():
            go(refs6[3:], 0, 'wait')

        return start, wait

    tiles_of = [ntiles[mb, row0 + e, 0] for e in range(E_RUN)]
    for e in range(E_RUN):
        rank = 0
        for o in range(E_RUN):
            if o != e:
                ahead = tiles_of[o] >= tiles_of[e] if o < e else tiles_of[o] > tiles_of[e]
                rank = rank + ahead.astype(i32)
        place = jnp.where(rank == 0, 0, jnp.where(rank == 1, E_RUN - 1, rank - 1))
        order[place] = e

    def clear(ref):
        rows = 64

        @pl.loop(0, ref.shape[0] // rows)
        def _(k):
            ref[pl.ds(pl.multiple_of(k * rows, rows), rows), :] = jnp.zeros((rows, ref.shape[1]), ref.dtype)

    w_start(order[0], 0)
    if carry:
        dw_copies(dw_in, order[0], 0, in_sem, True)[0]()
    clear(acc)
    for c in loads:
        c.wait()

    def window(e, st, k):
        size = WIN_MORE if k is not None else WIN
        so = starts[mb, row0 + e, st]
        if k is not None:
            so += WIN + (k - 1) * WIN_MORE
        s = jnp.minimum(so, n_tok - size)
        shift = lax.rem(s // ALIGN, 2)
        lanes = pl.ds(pl.multiple_of(s - shift * ALIGN, 128), size)
        rk = rank_ref[mb, shift, pl.ds(row0 + e, 1), lanes]
        lane = lax.broadcasted_iota(i32, (1, size), 1) + s
        rk = jnp.where(lane >= so, rk, -1) - st * SUB
        mask = lax.broadcasted_iota(i32, (SUB, size), 0) == rk
        toks = pl.ds(pl.multiple_of(s, ALIGN), size)
        return toks, lambda: jnp.where(mask, 1.0, 0.0).astype(bf16), \
            lambda: jnp.where(mask, gate_ref[mb, shift, pl.ds(row0 + e, 1), lanes], 0.0).astype(bf16)

    bounds = [0]
    for ref in p_out:
        bounds.append(bounds[-1] + ref.shape[0])

    def p_copy(q):
        for j, dst in enumerate(p_out):
            lo, hi = bounds[j] // OUT_ROWS, bounds[j + 1] // OUT_ROWS

            @pl.when((q >= lo) & (q < hi))
            def _():
                rows = pl.ds(pl.multiple_of((q - lo) * OUT_ROWS, OUT_ROWS), OUT_ROWS)
                src = acc.at[pl.ds(pl.multiple_of(q * OUT_ROWS, OUT_ROWS), OUT_ROWS), :]
                pltpu.make_async_copy(src, dst.at[rows, :], p_sem.at[j]).start()

    def expert(i, _):
        e = order[i]
        slot = lax.rem(i, 2)
        for c in w_copies(w_own, 0, slot):
            c.wait()

        @pl.when(i < E_RUN - 1)
        def _():
            w_start(order[i + 1], 1 - slot)

        wg, wu, wd = wg_buf.at[slot], wu_buf.at[slot], wd_buf.at[slot]
        if bwd:
            d_slot = lax.rem(i, DW_SLOTS)

            @pl.when(i >= 2)
            def _():
                dw_copies(dw_out, 0, lax.rem(i - 2, DW_SLOTS), out_sem, False)[1]()

            if carry:
                @pl.when(i < E_RUN - 1)
                def _():
                    dw_copies(dw_in, order[i + 1], lax.rem(i + 1, DW_SLOTS), in_sem, True)[0]()

                dw_copies(dw_in, e, d_slot, in_sem, True)[1]()
            else:
                for b in (dwg_buf, dwu_buf, dwd_buf):
                    clear(b.at[d_slot])
            dwg, dwu, dwd = dwg_buf.at[d_slot], dwu_buf.at[d_slot], dwd_buf.at[d_slot]

        def tile(t, _):
            for h in range(per_tile):
                rows = pl.ds(h * SUB, SUB)
                toks, ones, gated = window(e, t * per_tile + h, None)
                x_acc[rows, :] = dot_nn(ones(), tok[toks, :])
                if bwd:
                    d_acc[rows, :] = dot_nn(gated(), dyt[toks, :])

            n_win = nwins[mb, row0 + e, t * per_tile]
            for h in range(1, per_tile):
                n_win = jnp.maximum(n_win, nwins[mb, row0 + e, t * per_tile + h])

            @pl.when(n_win > 1)
            def _():
                @pl.loop(0, per_tile)
                def _(h):
                    st = t * per_tile + h
                    rows = pl.ds(pl.multiple_of(h * SUB, SUB), SUB)

                    @pl.loop(1, nwins[mb, row0 + e, st])
                    def _(k):
                        toks, ones, gated = window(e, st, k)
                        x_acc[rows, :] += dot_nn(ones(), tok[toks, :])
                        if bwd:
                            d_acc[rows, :] += dot_nn(gated(), dyt[toks, :])

            x = x_acc[...].astype(bf16)
            if bwd:
                d = d_acc[...].astype(bf16)
                xt[...] = x.T
            for c in range(0, ff, CHUNK):
                cols = pl.ds(c, CHUNK)
                gp = dot_nn(x, wg[:, cols]).astype(bf16).astype(f32)
                up = dot_nn(x, wu[:, cols]).astype(bf16).astype(f32)
                sig = 1.0 / (1.0 + jnp.exp(-gp))
                silu = gp * sig
                if not bwd:
                    act_all[:, cols] = (silu * up).astype(bf16)
                    continue
                da = dot_nt(d, wd[cols, :]).astype(bf16).astype(f32)
                act = (silu * up).astype(bf16)
                du = (da * silu).astype(bf16)
                dg = (da * up * (sig + silu * (1.0 - sig))).astype(bf16)
                dg_all[:, cols] = dg
                du_all[:, cols] = du
                dwd[cols, :] += dot_tn(act, d)
                dwg[:, cols] += dot_nn(xt[...], dg)
                dwu[:, cols] += dot_nn(xt[...], du)
            if bwd:
                out = (dot_nt(dg_all[...], wg[...]) + dot_nt(du_all[...], wu[...])).astype(bf16)
            else:
                out = dot_nn(act_all[...], wd[...]).astype(bf16)

            def put(st, k, part):
                toks, ones, gated = window(e, st, k)
                acc[toks, :] += dot_tn(ones() if bwd else gated(), part)

            out_all[...] = out
            for h in range(per_tile):
                put(t * per_tile + h, None, out[h * SUB:(h + 1) * SUB, :])

            @pl.when(n_win > 1)
            def _():
                @pl.loop(0, per_tile)
                def _(h):
                    st = t * per_tile + h

                    @pl.loop(1, nwins[mb, row0 + e, st])
                    def _(k):
                        put(st, k, out_all[pl.ds(pl.multiple_of(h * SUB, SUB), SUB), :])

            @pl.when(i == E_RUN - 1)
            def _():
                def final(tile_idx):
                    return jnp.minimum(starts[mb, row0 + e, tile_idx * per_tile], n_tok - WIN_MORE) // OUT_ROWS

                lo = jnp.where(t == 0, 0, final(t))
                hi = jnp.where(t == ntiles[mb, row0 + e, 0] - 1, n_tok // OUT_ROWS, final(t + 1))

                @pl.loop(lo, hi)
                def _(q):
                    p_copy(q)

            return 0

        lax.fori_loop(0, ntiles[mb, row0 + e, 0], tile, 0)
        if bwd:
            dw_copies(dw_out, e, d_slot, out_sem, False)[0]()
        return 0

    lax.fori_loop(0, E_RUN, expert, 0)
    outs = [pltpu.make_async_copy(acc.at[pl.ds(bounds[j], ref.shape[0]), :], ref, p_sem.at[j]) for j, ref in enumerate(p_out)]
    if bwd:
        for e in (E_RUN - 2, E_RUN - 1):
            dw_copies(dw_out, e, e % DW_SLOTS, out_sem, False)[1]()
    for c in outs:
        c.wait()


def routing_kernel(n_sub, who_ref, tab0, tab1, tab2, tab3, rank_ref, gate_ref, start_ref, nwin_ref, ntile_ref, hit_ref):
    fields, n_tok = tab0.shape
    top_k = fields // 4
    n2 = 2 * n_tok
    n_blk = n2 // 128
    r_i = lax.broadcasted_iota(i32, (128, 128), 0)
    c_i = lax.broadcasted_iota(i32, (128, 128), 1)
    tri = jnp.where(r_i <= c_i, 1.0, 0.0).astype(bf16)
    full = jnp.ones((128, 128), bf16)
    lane = lax.broadcasted_iota(i32, (2 * E_RUN, 128), 1)
    for mb in range(2):
        for q, tab in enumerate((tab0, tab1, tab2, tab3)):
            part = tab[mb * 2 * top_k:(mb + 1) * 2 * top_k, :]
            ids, gates = part[:top_k], part[top_k:]
            cols = pl.ds((q % 2) * n_tok, n_tok)
            for e in range(E_RUN):
                match = ids == who_ref[e].astype(f32)
                row = (q // 2) * E_RUN + e
                hit_ref[row:row + 1, cols] = jnp.sum(jnp.where(match, 1.0, 0.0), axis=0, keepdims=True)
                gate_ref[mb, 0, row:row + 1, cols] = jnp.sum(jnp.where(match, gates, 0.0), axis=0, keepdims=True)
        hits = [hit_ref[:, b * 128:(b + 1) * 128] for b in range(n_blk)]
        stacked = jnp.concatenate(hits, axis=0).astype(bf16)
        within = dot_nn(stacked, tri)
        totals = dot_nn(stacked, full)
        carry = jnp.zeros((2 * E_RUN, 128), f32)
        incl = []
        for b in range(n_blk):
            rows = slice(b * 2 * E_RUN, (b + 1) * 2 * E_RUN)
            v = (within[rows] + carry).astype(i32)
            rank_ref[mb, 0, :, b * 128:(b + 1) * 128] = jnp.where(hits[b] > 0.5, v - 1, -1)
            incl.append(v)
            carry = carry + totals[rows]
        for ref, fill in ((rank_ref, -1), (gate_ref, 0.0)):
            ref[mb, 1, :, :n2 - 128] = ref[mb, 0, :, ALIGN:n2 - 128 + ALIGN]
            tail = jnp.concatenate([ref[mb, 0, :, n2 - 128:], jnp.full((2 * E_RUN, 128), fill, ref.dtype)], axis=1)
            ref[mb, 1, :, n2 - 128:] = tail[:, ALIGN:128 + ALIGN]
        cnt = carry.astype(i32)

        def tokens_upto(limit):
            tot = jnp.zeros((2 * E_RUN, 128), f32)
            for v in incl:
                tot = tot + jnp.where(v <= limit, 1.0, 0.0)
            return jnp.sum(tot, axis=1, keepdims=True).astype(i32)

        start = jnp.zeros((2 * E_RUN, 128), i32)
        nwin = jnp.ones((2 * E_RUN, 128), i32)

        def one_sub(j, tables):
            start, nwin = tables
            lo = jnp.minimum(tokens_upto(j * SUB), n2 - 1) // ALIGN * ALIGN
            hi = tokens_upto(jnp.minimum((j + 1) * SUB, cnt) - 1) + 1
            n = jnp.maximum((hi - lo - WIN + WIN_MORE - 1) // WIN_MORE, 0) + 1
            return jnp.where(lane == j, lo, start), jnp.where(lane == j, n, nwin)

        start, nwin = lax.fori_loop(0, n_sub, one_sub, (start, nwin))
        start_ref[mb] = start
        nwin_ref[mb] = nwin
        tile_rows = SUB * TILE_SUBS[mb]
        ntile_ref[mb] = jnp.maximum((cnt + tile_rows - 1) // tile_rows, 1)


def run_routing(who, tables, n_sub):
    n_tok = tables[0].shape[1]
    rows = 2 * E_RUN
    wide = (2, 2, rows, 2 * n_tok)
    small = jax.ShapeDtypeStruct((2, rows, 128), i32)
    vmem = pl.BlockSpec(memory_space=pltpu.VMEM)
    return pl.pallas_call(
        functools.partial(routing_kernel, n_sub),
        out_shape=[jax.ShapeDtypeStruct(wide, i32), jax.ShapeDtypeStruct(wide, f32), small, small, small],
        in_specs=[pl.BlockSpec(memory_space=pltpu.SMEM)] + [vmem] * 4,
        out_specs=[vmem] * 5,
        scratch_shapes=[pltpu.VMEM((rows, 2 * n_tok), f32)],
        name='routing',
    )(who, *tables)


def sigmoid(v):
    return 1.0 / (1.0 + jnp.exp(-v))


def rms_scale(rows_f32):
    return lax.rsqrt(jnp.mean(rows_f32 * rows_f32, axis=-1, keepdims=True) + EPS_NORM)


def rms_back(rows_f32, cot):
    cot = cot.astype(f32)
    scale = rms_scale(rows_f32)
    proj = jnp.mean(cot * rows_f32, axis=-1, keepdims=True)
    return (scale * cot - rows_f32 * (scale * scale * scale * proj)).astype(bf16)


def dense_kernel(x_ref, w_in, w_out, norm_ref, mid_ref, *rest):
    *pre_ref, hid = rest
    x = x_ref[...].astype(f32)
    norm_in = (x * rms_scale(x)).astype(bf16)
    for c in range(0, w_in.shape[1], CHUNK):
        cols = pl.ds(c, CHUNK)
        pre = dot_nn(norm_in, w_in[:, cols]).astype(bf16)
        if pre_ref:
            pre_ref[0][:, cols] = pre
        pre = pre.astype(f32)
        hid[:, cols] = (pre * sigmoid(pre)).astype(bf16)
    mid = (x_ref[...].astype(f32) + dot_nn(hid[...], w_out[...])).astype(bf16)
    mid_ref[...] = mid
    mid = mid.astype(f32)
    norm_ref[...] = (mid * rms_scale(mid)).astype(bf16)


def run_dense(x, w_in, w_out, keep_pre):
    n_tok, width = x.shape
    ff = w_in.shape[1]
    row = pl.BlockSpec((DENSE_ROWS, width), lambda i: (i, 0))
    out_shape = [jax.ShapeDtypeStruct(x.shape, bf16)] * 2
    out_specs = [row, row]
    if keep_pre:
        out_shape += [jax.ShapeDtypeStruct((n_tok, ff), bf16)]
        out_specs += [pl.BlockSpec((DENSE_ROWS, ff), lambda i: (i, 0))]
    return pl.pallas_call(
        dense_kernel,
        grid=(n_tok // DENSE_ROWS,),
        out_shape=out_shape,
        in_specs=[row, pl.BlockSpec((width, ff), lambda i: (0, 0)), pl.BlockSpec((ff, width), lambda i: (0, 0))],
        out_specs=out_specs,
        scratch_shapes=[pltpu.VMEM((DENSE_ROWS, ff), bf16)],
        cost_estimate=pl.CostEstimate(flops=4 * n_tok * width * ff, bytes_accessed=12_000_000, transcendentals=0),
        name='dense_fwd',
    )(x, w_in, w_out)


def tail_kernel(p_own, p_mate, p_far, mid_ref, dy_ref, x_ref, pre_ref, w_in, w_out, dx_ref, d_all):
    d_norm = (p_own[...] + p_mate[...] + p_far[...]).astype(bf16)
    d_mid = (dy_ref[...].astype(f32) + rms_back(mid_ref[...].astype(f32), d_norm).astype(f32)).astype(bf16)
    for c in range(0, w_in.shape[1], CHUNK):
        cols = pl.ds(c, CHUNK)
        d_hid = dot_nt(d_mid, w_out[cols, :]).astype(bf16).astype(f32)
        pre = pre_ref[:, cols].astype(f32)
        sig = sigmoid(pre)
        d_all[:, cols] = (d_hid * (sig + pre * sig * (1.0 - sig))).astype(bf16)
    d_in = dot_nt(d_all[...], w_in[...]).astype(bf16)
    dx_ref[...] = (d_mid.astype(f32) + rms_back(x_ref[...].astype(f32), d_in).astype(f32)).astype(bf16)


def run_tail(chunk, p_own, p_mate, p_far, mid, dy, x, pre, w_in, w_out):
    n_tok, width = x.shape
    ff = w_in.shape[1]
    first, steps = TAIL[chunk], TAIL[chunk + 1] - TAIL[chunk]
    rows = n_tok // TAIL[-1]
    row = pl.BlockSpec((rows, width), lambda i: (first + i, 0))
    return pl.pallas_call(
        tail_kernel,
        grid=(steps,),
        out_shape=jax.ShapeDtypeStruct((rows * steps, width), bf16),
        in_specs=[row, pl.BlockSpec((rows, width), lambda i: (first + i if chunk == 0 else first + i - OUT_ROWS // rows, 0))] + [row] * 4 + [pl.BlockSpec((rows, ff), lambda i: (first + i, 0)),
                              pl.BlockSpec((width, ff), lambda i: (0, 0)), pl.BlockSpec((ff, width), lambda i: (0, 0))],
        out_specs=pl.BlockSpec((rows, width), lambda i: (i, 0)),
        scratch_shapes=[pltpu.VMEM((rows, ff), bf16)],
        cost_estimate=pl.CostEstimate(flops=4 * rows * steps * width * ff, bytes_accessed=6_000_000, transcendentals=0),
    )(p_own, p_mate, p_far, mid, dy, x, pre, w_in, w_out)


def run_experts(meta, far, toks, dys, w_own, w_mate, dw_prev):
    starts, nwins, ntiles, base, rank, gate = meta
    bwd = dys is not None
    carry = dw_prev is not None
    half, width = toks[0].shape
    e_loc, _, ff = w_own[0].shape
    smem = pl.BlockSpec(memory_space=pltpu.SMEM)
    vmem = pl.BlockSpec(memory_space=pltpu.VMEM)
    hbm = pl.BlockSpec(memory_space=pl.ANY)
    args = [starts, nwins, ntiles, base, rank, gate, *toks]
    if bwd:
        args += [*dys]
    args += [*w_own, *w_mate]
    if carry:
        args += [*dw_prev]
    in_specs = [smem] * 4 + [vmem] * 2 + [hbm] * (len(args) - 6)
    p_rows = [half, OUT_ROWS, half - OUT_ROWS] if carry else [half, half]
    out_shape = [jax.ShapeDtypeStruct((n, width), f32) for n in p_rows]
    if bwd:
        for n in (e_loc, 2):
            out_shape += [jax.ShapeDtypeStruct((n, *w.shape[1:]), f32) for w in w_own]
    rows = SUB * TILE_SUBS[int(bwd)]
    scratch = [
        pltpu.SMEM((E_RUN,), i32),
        pltpu.VMEM((2 * half, width), bf16),
        pltpu.VMEM((2 * half, width), f32),
        pltpu.VMEM((2, width, ff), bf16),
        pltpu.VMEM((2, width, ff), bf16),
        pltpu.VMEM((2, ff, width), bf16),
        pltpu.VMEM((rows, width), f32),
        pltpu.VMEM((rows, width), bf16),
    ]
    if bwd:
        scratch += [
            pltpu.VMEM((2 * half, width), bf16),
            pltpu.VMEM((rows, width), f32),
            pltpu.VMEM((width, rows), bf16),
            pltpu.VMEM((rows, ff), bf16),
            pltpu.VMEM((rows, ff), bf16),
            pltpu.VMEM((DW_SLOTS, width, ff), f32),
            pltpu.VMEM((DW_SLOTS, width, ff), f32),
            pltpu.VMEM((DW_SLOTS, ff, width), f32),
            pltpu.SemaphoreType.DMA((2, 2)),
            pltpu.SemaphoreType.DMA((2, 3)),
            pltpu.SemaphoreType.DMA((3,)),
            pltpu.SemaphoreType.DMA((DW_SLOTS, 3)),
            pltpu.SemaphoreType.DMA((DW_SLOTS, 3)),
        ]
    else:
        scratch += [
            pltpu.VMEM((rows, ff), bf16),
            pltpu.SemaphoreType.DMA((2, 2)),
            pltpu.SemaphoreType.DMA((2, 3)),
            pltpu.SemaphoreType.DMA((3,)),
        ]
    flops = (8 if bwd else 3) * 2 * 3584 * 2 * width * ff
    return pl.pallas_call(
        functools.partial(expert_kernel, bwd, carry, E_RUN if far else 0, len(p_rows)),
        out_shape=out_shape,
        in_specs=in_specs,
        out_specs=[hbm] * len(out_shape),
        scratch_shapes=scratch,
        compiler_params=pltpu.CompilerParams(vmem_limit_bytes=60 * 1024 * 1024),
        cost_estimate=pl.CostEstimate(flops=flops, bytes_accessed=60_000_000, transcendentals=0),
        name='experts_bwd' if bwd else 'experts_fwd',
    )(*args)


def solution(mesh):
    n_ep = mesh.shape['ep']
    n_pp = mesh.shape['pp']
    n_tail = len(TAIL) - 1
    fwd_perm = [(i, (i + 1) % n_pp) for i in range(n_pp)]
    bwd_perm = [(i, (i - 1) % n_pp) for i in range(n_pp)]

    def to_mate(v):
        return lax.ppermute(v, 'ep', [(i, i ^ 1) for i in range(n_ep)])

    def to_cross(v):
        return lax.ppermute(v, 'ep', [(i, i ^ 2) for i in range(n_ep)])

    def device_fn(x_fwd, x_bwd, dy_bwd, ids_fwd, gate_fwd, ids_bwd, gate_bwd, w_in, w_out, w_gate, w_up, w_down):
        fwd_x, bwd_x, bwd_dy = x_fwd[0], x_bwd[0], dy_bwd[0]
        stage_w_in, stage_w_out = w_in[0], w_out[0]
        w_own = (w_gate[0], w_up[0], w_down[0])
        n_tok, _ = fwd_x.shape
        top_k = ids_fwd.shape[2]
        e_loc = w_own[0].shape[0]
        n_exp = e_loc * n_ep
        cap = 3 * n_tok * top_k // n_exp
        me = lax.axis_index('ep')
        core = lax.rem(me, 2)
        base = 2 * core
        n_sub = -(-2 * cap // SUB)

        def gather_pair(v):
            far = to_cross(v)
            return (v, to_mate(v)), (far, to_mate(far))

        fields = [ids_fwd[0].astype(f32).T, gate_fwd[0].astype(f32).T, ids_bwd[0].astype(f32).T, gate_bwd[0].astype(f32).T]
        table = jnp.concatenate(fields)
        tables = [table, to_mate(table), to_cross(table)]
        tables.append(lax.ppermute(table, 'ep', [(i, i ^ 3) for i in range(n_ep)]))
        mine = e_loc * me + base
        mates = e_loc * (me ^ 1) + base
        who = jnp.stack([mine, mine + 1, mates, mates + 1]).astype(i32)
        base_arr = base.reshape(1).astype(i32)
        ranks, gates, starts, nwins, ntiles = run_routing(who, tables, n_sub)
        meta = (starts, nwins, ntiles, base_arr, ranks, gates)

        far_dy = to_cross(bwd_dy)
        dy_near, dy_far = (bwd_dy, to_mate(bwd_dy)), (far_dy, to_mate(far_dy))
        w_mate = tuple(to_mate(w) for w in w_own)

        def combine(parts):
            return parts[0] + to_mate(parts[1])

        norm_f, mid_f = run_dense(fwd_x, stage_w_in, stage_w_out, False)
        near_f, far_f = gather_pair(norm_f)
        norm_b, mid_b, pre_b = run_dense(bwd_x, stage_w_in, stage_w_out, True)
        near_b, far_b = gather_pair(norm_b)

        pf_near = run_experts(meta, False, near_f, None, w_own, w_mate, None)
        pf_far = run_experts(meta, True, far_f, None, w_own, w_mate, None)
        ret_f = to_cross(combine(pf_far))
        pb_far = run_experts(meta, True, far_b, dy_far, w_own, w_mate, None)
        ret_b = to_cross(combine(pb_far[:2]))
        pb_near = run_experts(meta, False, near_b, dy_near, w_own, w_mate, pb_far[2:])
        dw_full, dw_mate = pb_near[3:6], pb_near[6:9]

        near_f_mate = to_mate(pf_near[1])
        y_val = (mid_f.astype(f32) + (pf_near[0] + near_f_mate + ret_f)).astype(bf16)
        y_next = lax.ppermute(y_val, 'pp', fwd_perm)

        dx_parts = []
        from_mate = [to_mate(pb_near[1 + k]) for k in range(2)]
        for c in range(n_tail):
            dx_val = run_tail(c, pb_near[0], from_mate[min(c, 1)], ret_b, mid_b, bwd_dy, bwd_x, pre_b, stage_w_in, stage_w_out)
            dx_parts.append(lax.ppermute(dx_val, 'pp', bwd_perm))
        dx_prev = jnp.concatenate(dx_parts)

        back = [to_mate(v) for v in dw_mate]
        zero = jnp.zeros((), i32)
        dw_gate, dw_up, dw_down = [lax.dynamic_update_slice(full, part, (2 - base, zero, zero)) for full, part in zip(dw_full, back)]
        return y_next[None], dx_prev[None], dw_gate[None], dw_up[None], dw_down[None]

    spec_act = P('pp', 'ep', None)
    spec_dense = P('pp', None, None)
    spec_exp = P('pp', 'ep', None, None)


    return jax.shard_map(device_fn, mesh=mesh, in_specs=(spec_act,) * 7 + (spec_dense,) * 2 + (spec_exp,) * 3, out_specs=(spec_act, spec_act, spec_exp, spec_exp, spec_exp), check_vma=False)
```
